32 devices in a mesh: rep: 1 (over z), tp: 4 (over y), dp: 8 (over x, core).
Axes of the slice: x: 4, y: 4, z: 1, core: 2. Of those that a mesh axis runs over, the one named last changes fastest.
The devices are a block of a 4x4x8 slice.
Arguments:
- grad_partial: float32 [8, 8, 1024, 2048], P(('rep', 'dp'), None, None, 'tp')
- momentum: float32 [8, 1024, 2048], P('rep', 'dp', 'tp')
- weight: float32 [8, 1024, 2048], P('rep', 'dp', 'tp')
- learn_rate: float32 [8], P('rep')
- decay_rate: float32 [], replicated
Outputs:
- output 1: float32 [8, 1024, 2048], P('rep', 'dp', 'tp')
- output 2: float32 [8, 1024, 2048], P('rep', 'dp', 'tp')
- output 3: bfloat16 [8, 1024, 2048], P('rep', None, 'tp')
All inputs are finite; a program needn't handle non-finite values.
Results may differ from the reference program's by a relative error of at most 0.0131368.
Values are sent between devices in bfloat16 or wider.
A program may use at most 768 MiB of HBM per device.

```python
import math
import jax
import jax.numpy as jnp
from jax import lax

DP_SIZE = 8
MATS = 8
ROWS = 1024
COLS = 2048

MOMENTUM = 0.95
NS_STEPS = 5
COEF_A = 3.4445
COEF_B = -4.7750
COEF_C = 2.0315
NORM_EPS = 1e-7
OUT_SCALE = 0.2 * math.sqrt(max(ROWS, COLS))


def setup_inputs(seed: int = 0, part: int = 0) -> dict:
    part_key = jax.random.fold_in(jax.random.key(seed), part)
    key_grad, key_scale, key_mom, key_weight, key_rate = jax.random.split(part_key, 5)
    key_decay = jax.random.key(seed + 1)
    dev_scale = jax.random.uniform(key_scale, (DP_SIZE, 1, 1, 1), minval=0.5, maxval=2.0)
    grad_partial = jax.random.normal(key_grad, (DP_SIZE, MATS, ROWS, COLS)) * dev_scale * math.sqrt(DP_SIZE)
    momentum = jax.random.normal(key_mom, (MATS, ROWS, COLS))
    weight = 0.25 * jax.random.normal(key_weight, (MATS, ROWS, COLS))
    learn_rate = jax.random.uniform(key_rate, (MATS,), minval=0.1, maxval=1.0)
    decay_rate = jax.random.uniform(key_decay, (), minval=0.2, maxval=0.5)
    return {
        "grad_partial": grad_partial.astype(jnp.float32),
        "momentum": momentum.astype(jnp.float32),
        "weight": weight.astype(jnp.float32),
        "learn_rate": learn_rate.astype(jnp.float32),
        "decay_rate": decay_rate.astype(jnp.float32),
    }


def orthogonalize(update):
    upd_f32 = update.astype(jnp.float32)
    norm_val = jnp.sqrt(jnp.sum(upd_f32 * upd_f32))
    x_cur = (upd_f32 / (norm_val + NORM_EPS)).astype(jnp.bfloat16)
    if ROWS > COLS:
        x_cur = x_cur.T
    for step_idx in range(NS_STEPS):
        gram_mat = jnp.dot(x_cur, x_cur.T, preferred_element_type=jnp.float32).astype(jnp.bfloat16)
        gram_sq = jnp.dot(gram_mat, gram_mat, preferred_element_type=jnp.float32)
        poly_mat = (COEF_B * gram_mat.astype(jnp.float32) + COEF_C * gram_sq).astype(jnp.bfloat16)
        prod_mat = jnp.dot(poly_mat, x_cur, preferred_element_type=jnp.float32)
        x_cur = (COEF_A * x_cur.astype(jnp.float32) + prod_mat).astype(jnp.bfloat16)
    if ROWS > COLS:
        x_cur = x_cur.T
    return x_cur


def reference(grad_partial, momentum, weight, learn_rate, decay_rate):
    grad_mean = jnp.mean(grad_partial, axis=0)
    mom_new = MOMENTUM * momentum + grad_mean
    update = (grad_mean + MOMENTUM * mom_new).astype(jnp.bfloat16)
    ortho_mat = lax.map(orthogonalize, update)
    rate_col = learn_rate[:, None, None]
    weight_new = weight - rate_col * (OUT_SCALE * ortho_mat.astype(jnp.float32) + decay_rate * weight)
    return mom_new, weight_new, weight_new.astype(jnp.bfloat16)
```

```python
import functools
import math

import jax
import jax.numpy as jnp
from jax import lax
from jax.experimental import pallas as pl
from jax.experimental.pallas import tpu as pltpu
from jax.sharding import PartitionSpec as P

MOMENTUM = 0.95
NS_STEPS = 5
COEF_A = 3.4445
COEF_B = -4.7750
COEF_C = 2.0315
NORM_EPS = 1e-7
MESH = pl.DeviceIdType.MESH
F32 = jnp.float32
BF16 = jnp.bfloat16
CHUNKS = 4


def dot_nt(lhs, rhs):
    return lax.dot_general(lhs, rhs, (((1,), (1,)), ((), ())), preferred_element_type=F32)


def dot_nn(lhs, rhs):
    return jnp.dot(lhs, rhs, preferred_element_type=F32)


def muon_kernel(
    dims, grad, mom, wgt, rate, decay, mom_out, wgt_out, full_out,
    gown, gpar, ring, momv, usend, xs, aown, apar, bmat, xfin, wgtv, xback, full,
    own_sem, mw_sem, out_sem, gp_s, gp_r, ring_s, ring_r, a2a_s, a2a_r, yg_s, yg_r, half_s, half_r,
    xe_s, xe_r, ae_s, ae_r, bk_s, bk_r, ag_s, ag_r, ad_s, ad_r,
):
    nx, tp, mats, rows, cols = dims
    waves = mats // nx
    piece = rows // CHUNKS
    half = nx * rows
    width = tp * cols
    blk = min(256, half // 2)
    nblk = min(256, cols // 2)
    out_scale = 0.2 * math.sqrt(max(2 * half, width))

    d = lax.axis_index("dp")
    y = lax.axis_index("tp")
    x = d // 2
    c = d % 2
    turn = 1 - 2 * c
    nxt_x = (x + turn + nx) % nx
    partner = {"dp": 2 * x + (1 - c)}
    right = {"dp": 2 * nxt_x + c}

    def at_x(dx):
        return {"dp": 2 * ((x + dx) % nx) + c}

    def at_y(dy):
        return {"tp": (y + dy) % tp}

    def remote(src, dst, send, recv, dev):
        return pltpu.make_async_remote_copy(
            src_ref=src, dst_ref=dst, send_sem=send, recv_sem=recv, device_id=dev, device_id_type=MESH
        )

    def wave(w):
        return pl.ds(w * nx, nx)

    def part(q):
        return pl.ds(q * piece, piece)

    def own_load(w, q):
        return pltpu.make_async_copy(
            grad.at[wave(w), :, c, part(q)], gown.at[wave(w), :, part(q)], own_sem.at[w, q]
        )

    def pair_copy(w, q):
        return remote(
            grad.at[wave(w), :, 1 - c, part(q)], gpar.at[wave(w), :, part(q)], gp_s.at[w, q], gp_r.at[w, q], partner
        )

    mom_load = pltpu.make_async_copy(mom, momv, mw_sem.at[0])
    wgt_load = pltpu.make_async_copy(wgt, wgtv, mw_sem.at[1])
    for w in range(waves):
        for q in range(CHUNKS):
            own_load(w, q).start()
    mom_load.start()
    wgt_load.start()

    barrier = pltpu.get_barrier_semaphore()
    peers = [partner] + [at_x(dx) for dx in range(1, nx)] + [at_y(dy) for dy in range(1, tp)]
    for peer in peers:
        pl.semaphore_signal(barrier, inc=1, device_id=peer, device_id_type=MESH)
    pl.semaphore_wait(barrier, len(peers))
    for w in range(waves):
        for q in range(CHUNKS):
            pair_copy(w, q).start()

    def ring_block(stage):
        return (x - turn * (1 + stage) + 4 * nx) % nx

    def ring_copy(w, q, stage):
        if stage == 0:
            src = gown.at[wave(w), ring_block(0), part(q)]
        else:
            src = ring.at[w, q, stage - 1]
        return remote(src, ring.at[w, q, stage], ring_s.at[w, q, stage], ring_r.at[w, q, stage], right)

    def a2a_copy(w, q, dx):
        owner = (x + dx) % nx
        return remote(
            usend.at[w * nx + owner, part(q)],
            xs.at[w, pl.ds(pl.multiple_of(x * rows + q * piece, piece), piece),
                  pl.ds(pl.multiple_of(y * cols, cols), cols)],
            a2a_s.at[w, q, dx], a2a_r.at[w, q, dx], at_x(dx),
        )

    def ring_event(w, q, stage):
        block = ring_block(stage)
        if stage == 0:
            own_load(w, q).wait()
            pair_copy(w, q).wait_recv()
        else:
            ring_copy(w, q, stage - 1).wait_recv()
        for i in range(nx):
            m = w * nx + i
            local = gown[m, block, part(q)] + gpar[m, block, part(q)]
            if stage == 0:
                gown[m, block, part(q)] = local
            elif stage < nx - 1:
                ring[w, q, stage - 1, i] = ring[w, q, stage - 1, i] + local
            else:
                grad_mean = (ring[w, q, stage - 1, i] + local) * (1.0 / (2 * nx))
                mom_new = MOMENTUM * momv[m, part(q)] + grad_mean
                momv[m, part(q)] = mom_new
                usend[m, part(q)] = (grad_mean + MOMENTUM * mom_new).astype(BF16)
        if stage < nx - 1:
            ring_copy(w, q, stage).start()
        else:
            for dx in (2, 1, 3):
                a2a_copy(w, q, dx).start()
            xs[w, pl.ds(pl.multiple_of(x * rows + q * piece, piece), piece),
               pl.ds(pl.multiple_of(y * cols, cols), cols)] = usend[w * nx + x, part(q)]

    def gather_copy(w, q, dy, i):
        region = xs.at[w, pl.ds(i * rows + q * piece, piece), pl.ds(pl.multiple_of(y * cols, cols), cols)]
        return remote(region, region, yg_s.at[w, q, dy - 1, i], yg_r.at[w, q, dy - 1, i], at_y(dy))

    def half_copy(w, q, i):
        return remote(
            xs.at[w, pl.ds(i * rows + q * piece, piece)],
            xs.at[w, pl.ds(half + i * rows + q * piece, piece)],
            half_s.at[w, q, i], half_r.at[w, q, i], partner,
        )

    def gather_event(w, q):
        for dx in (1, 3, 2):
            a2a_copy(w, q, dx).wait_recv()
        for dy in (2, 1, 3):
            if dy < tp:
                for i in range(nx):
                    gather_copy(w, q, dy, i).start()

    def half_event(w, q):
        for dy in (1, 3, 2):
            if dy < tp:
                for i in range(nx):
                    gather_copy(w, q, dy, i).wait_recv()
        for i in range(nx):
            half_copy(w, q, i).start()

    strip = 64

    def normalise(w):
        for q in range(CHUNKS):
            for i in range(nx):
                half_copy(w, q, i).wait_recv()
                half_copy(w, q, i).wait_send()
        for q in range(CHUNKS):
            for dy in range(1, tp):
                for i in range(nx):
                    gather_copy(w, q, dy, i).wait_send()

        def add_squares(r, acc):
            v = xs[w, pl.ds(pl.multiple_of(r * 16, 16), 16), :].astype(F32)
            v = v * v
            return acc + v

        total = jnp.sum(lax.fori_loop(0, 2 * half // 16, add_squares, jnp.zeros((16, width), F32)))
        inv = 1.0 / (jnp.sqrt(jnp.full((8, 128), total, F32)) + NORM_EPS)
        inv = inv[0:1, 0:1]

        def scale_rows(r, carry):
            sl = pl.ds(pl.multiple_of(r * 16, 16), 16)
            xs[w, sl, :] = (xs[w, sl, :].astype(F32) * inv).astype(BF16)
            return carry

        lax.fori_loop(0, 2 * half // 16, scale_rows, 0)

    own = pl.ds(0, half)

    def chunk_copy(dst, par, n):
        col = pl.ds(pl.multiple_of(n * nblk, nblk), nblk)
        return remote(
            xs.at[dst, own, col], xs.at[dst, pl.ds(half, half), col], xe_s.at[par, n], xe_r.at[par, n], partner
        )

    n_chunks = width // nblk

    def newton_schulz(w, service):
        def a_copy(par):
            return remote(aown.at[:, own], apar.at[par], ae_s.at[par], ae_r.at[par], partner)

        def body(it, carry):
            par = it % 2
            cur = jnp.where(par == 0, w, waves)
            nxt = jnp.where(par == 0, waves, w)

            def a_block(j, cc):
                rs = pl.ds(pl.multiple_of(j * blk, blk), blk)
                aown[:, rs] = dot_nt(xs[cur, own, :], xs[cur, rs, :]).astype(BF16)
                return cc

            @pl.when(it > 0)
            def _():
                a_copy(1 - par).wait_send()

            lax.fori_loop(0, half // blk, a_block, 0)
            a_copy(par).start()
            service(it, 0)

            @pl.when(it > 0)
            def _():
                for n in range(n_chunks):
                    chunk_copy(cur, 1 - par, n).wait()

            lax.fori_loop(half // blk, 2 * half // blk, a_block, 0)
            service(it, 1)

            def b_own(j, cc):
                rs = pl.ds(pl.multiple_of(j * blk, blk), blk)
                sq = dot_nt(aown[...], aown[rs, :])
                bmat[:, rs] = (COEF_B * aown[:, rs].astype(F32) + COEF_C * sq).astype(BF16)
                return cc

            def b_other(j, cc):
                rs = pl.ds(pl.multiple_of(j * blk, blk), blk)
                ps = pl.ds(pl.multiple_of(half + j * blk, blk), blk)
                sq = dot_nn(aown[:, :half], aown[:, ps]) + dot_nn(aown[:, half:], apar[par, :, rs])
                bmat[:, ps] = (COEF_B * aown[:, ps].astype(F32) + COEF_C * sq).astype(BF16)
                return cc

            lax.fori_loop(0, half // blk, b_own, 0)
            a_copy(par).wait_recv()
            lax.fori_loop(0, half // blk, b_other, 0)
            service(it, 2)

            def x_block(n, cc):
                col = pl.ds(pl.multiple_of(n * nblk, nblk), nblk)
                new = COEF_A * xs[cur, own, col].astype(F32) + dot_nn(bmat[...], xs[cur, :, col])
                xs[nxt, own, col] = new.astype(BF16)
                chunk_copy(nxt, par, n).start()
                return cc

            def x_last(n, cc):
                col = pl.ds(pl.multiple_of(y * cols + n * nblk, nblk), nblk)
                new = COEF_A * xs[cur, own, col].astype(F32) + dot_nn(bmat[...], xs[cur, :, col])
                xfin[w, :, pl.ds(pl.multiple_of(n * nblk, nblk), nblk)] = new.astype(BF16)
                return cc

            @pl.when(it < NS_STEPS - 1)
            def _():
                lax.fori_loop(0, n_chunks, x_block, 0)

            @pl.when(it == NS_STEPS - 1)
            def _():
                lax.fori_loop(0, cols // nblk, x_last, 0)

            service(it, 3)
            return carry

        lax.fori_loop(0, NS_STEPS, body, 0)
        a_copy((NS_STEPS - 1) % 2).wait_send()

    def back_copy(w, dx):
        return remote(
            xfin.at[w, pl.ds(pl.multiple_of((x + dx) % nx * rows, rows), rows)],
            xback.at[w * nx + x], bk_s.at[w, dx], bk_r.at[w, dx], at_x(dx),
        )

    def back_arrival(w, dx):
        m = w * nx + (x - dx + nx) % nx
        return remote(
            xfin.at[w, pl.ds(0, rows)], xback.at[m], bk_s.at[w, dx], bk_r.at[w, dx], at_x(dx)
        )

    def back_send(w):
        for dx in (2, 1, 3):
            back_copy(w, dx).start()
        xback[w * nx + x] = xfin[w, pl.ds(pl.multiple_of(x * rows, rows), rows)]

    order = (0, 1, 3, 2)

    def gather_slot(w, hop, j):
        holder = (x - turn * hop + 4 * nx) % nx
        return holder, w * nx + (holder - order[j] + nx) % nx

    def ag_copy(w, hop, j):
        holder, m = gather_slot(w, hop, j)
        block = full.at[m, holder, c]
        return remote(block, block, ag_s.at[m, hop], ag_r.at[m, hop], right)

    def ag_arrival(w, hop, j):
        holder, m = gather_slot(w, hop + 1, j)
        block = full.at[m, holder, c]
        return remote(block, block, ag_s.at[m, hop], ag_r.at[m, hop], right)

    def pair_full(w, hop, j):
        holder, m = gather_slot(w, hop, j)
        block = full.at[m, holder, c]
        return remote(block, block, ad_s.at[m, hop], ad_r.at[m, hop], partner)

    def pair_arrival(w, hop, j):
        holder = (x + turn * hop + 4 * nx) % nx
        m = w * nx + (holder - order[j] + nx) % nx
        block = full.at[m, holder, 1 - c]
        return remote(block, block, ad_s.at[m, hop], ad_r.at[m, hop], partner)

    def weight_event(w, j):
        dx = order[j]
        m = w * nx + (x - dx + nx) % nx
        if dx:
            back_arrival(w, dx).wait_recv()
        w_old = wgtv[m]
        w_new = w_old - rate[m] * (out_scale * xback[m].astype(F32) + decay[0] * w_old)
        wgtv[m] = w_new
        full[m, x, c] = w_new.astype(BF16)
        ag_copy(w, 0, j).start()
        pair_full(w, 0, j).start()

    def forward_event(w, hop, j):
        ag_arrival(w, hop - 1, j).wait_recv()
        if hop < nx - 1:
            ag_copy(w, hop, j).start()
        pair_full(w, hop, j).start()

    def finish_gather(w):
        for hop in range(nx):
            for j in range(nx):
                pair_arrival(w, hop, j).wait_recv()
        full_store(w).start()

    def full_store(w):
        return pltpu.make_async_copy(full.at[wave(w)], full_out.at[wave(w)], out_sem.at[w, 0])

    def mom_store(w):
        return pltpu.make_async_copy(momv.at[wave(w)], mom_out.at[wave(w)], out_sem.at[w, 1])

    def wgt_store(w):
        return pltpu.make_async_copy(wgtv.at[wave(w)], wgt_out.at[wave(w)], out_sem.at[w, 2])

    last = nx - 1
    for q, stage in ((0, 0), (1, 0), (0, 1), (1, 1), (0, 2), (1, 2), (2, 0), (3, 0)):
        ring_event(0, q, stage)
    mom_load.wait()
    ring_event(0, 0, last)
    ring_event(0, 1, last)
    ring_event(0, 2, 1)
    ring_event(0, 3, 1)
    gather_event(0, 0)
    gather_event(0, 1)
    ring_event(0, 2, 2)
    ring_event(0, 3, 2)
    for q in range(CHUNKS):
        ring_event(1, q, 0)
    half_event(0, 0)
    half_event(0, 1)
    ring_event(0, 2, last)
    ring_event(0, 3, last)
    mom_store(0).start()
    gather_event(0, 2)
    gather_event(0, 3)
    half_event(0, 2)
    half_event(0, 3)
    normalise(0)

    def serve_first(it, slot):
        @pl.when(it == 0)
        def _():
            ring_event(1, slot, 1)

        @pl.when(it == 2)
        def _():
            ring_event(1, slot, 2)

        @pl.when(it == 4)
        def _():
            ring_event(1, slot, last)

    newton_schulz(0, serve_first)
    back_send(0)
    mom_store(1).start()
    for q in range(CHUNKS):
        gather_event(1, q)
    wgt_load.wait()
    for j in range(nx):
        weight_event(0, j)
    wgt_store(0).start()
    for q in range(CHUNKS):
        half_event(1, q)
    normalise(1)

    def serve_second(it, slot):
        for hop in (1, 2, 3):
            @pl.when(it == hop - 1)
            def _(hop=hop):
                forward_event(0, hop, slot)

        if slot == 3:
            @pl.when(it == 3)
            def _():
                finish_gather(0)

    newton_schulz(1, serve_second)
    back_send(1)
    for j in range(nx):
        weight_event(1, j)
    wgt_store(1).start()
    for hop in range(1, nx):
        for j in range(nx):
            forward_event(1, hop, j)
    finish_gather(1)

    for w in range(waves):
        for q in range(CHUNKS):
            pair_copy(w, q).wait_send()
            for stage in range(nx - 1):
                ring_copy(w, q, stage).wait_send()
            for dx in range(1, nx):
                a2a_copy(w, q, dx).wait_send()
        for dx in range(1, nx):
            back_copy(w, dx).wait_send()
        for hop in range(nx):
            for j in range(nx):
                if hop < nx - 1:
                    ag_copy(w, hop, j).wait_send()
                pair_full(w, hop, j).wait_send()
        mom_store(w).wait()
        wgt_store(w).wait()
        full_store(w).wait()


def solution(mesh):
    dp = mesh.shape["dp"]
    tp = mesh.shape["tp"]
    nx = dp // 2

    def local_step(grad_local, mom_local, weight_local, learn_rate, decay_rate):
        mats, rows, cols = mom_local.shape
        waves = mats // nx
        piece = rows // CHUNKS
        half = nx * rows
        width = tp * cols
        n_chunks = width // min(256, cols // 2)
        dma = pltpu.SemaphoreType.DMA
        vmem = pltpu.VMEM
        anyspec = pl.BlockSpec(memory_space=pl.ANY)
        smem = pl.BlockSpec(memory_space=pltpu.SMEM)
        grad_view = grad_local.reshape(mats, nx, 2, rows, cols)
        call = pl.pallas_call(
            functools.partial(muon_kernel, (nx, tp, mats, rows, cols)),
            out_shape=(
                jax.ShapeDtypeStruct((mats, rows, cols), F32),
                jax.ShapeDtypeStruct((mats, rows, cols), F32),
                jax.ShapeDtypeStruct((mats, nx, 2, rows, cols), BF16),
            ),
            in_specs=[anyspec, anyspec, anyspec, smem, smem],
            out_specs=(anyspec, anyspec, anyspec),
            scratch_shapes=[
                vmem((mats, nx, rows, cols), F32),
                vmem((mats, nx, rows, cols), F32),
                vmem((waves, CHUNKS, nx - 1, nx, piece, cols), F32),
                vmem((mats, rows, cols), F32),
                vmem((mats, rows, cols), BF16),
                vmem((waves + 1, 2 * half, width), BF16),
                vmem((half, 2 * half), BF16),
                vmem((2, half, half), BF16),
                vmem((half, 2 * half), BF16),
                vmem((waves, half, cols), BF16),
                vmem((mats, rows, cols), F32),
                vmem((mats, rows, cols), BF16),
                vmem((mats, nx, 2, rows, cols), BF16),
                dma((waves, CHUNKS)),
                dma((2,)),
                dma((waves, 3)),
                dma((waves, CHUNKS)),
                dma((waves, CHUNKS)),
                dma((waves, CHUNKS, nx - 1)),
                dma((waves, CHUNKS, nx - 1)),
                dma((waves, CHUNKS, nx)),
                dma((waves, CHUNKS, nx)),
                dma((waves, CHUNKS, tp - 1, nx)),
                dma((waves, CHUNKS, tp - 1, nx)),
                dma((waves, CHUNKS, nx)),
                dma((waves, CHUNKS, nx)),
                dma((2, n_chunks)),
                dma((2, n_chunks)),
                dma((2,)),
                dma((2,)),
                dma((waves, nx)),
                dma((waves, nx)),
                dma((mats, nx)),
                dma((mats, nx)),
                dma((mats, nx)),
                dma((mats, nx)),
            ],
            compiler_params=pltpu.CompilerParams(
                collective_id=0, has_side_effects=True, vmem_limit_bytes=64 * 1024 * 1024 - 65536
            ),
        )
        mom_new, weight_new, full = call(
            grad_view, mom_local, weight_local, learn_rate, decay_rate.reshape(1)
        )
        return mom_new, weight_new, full.reshape(mats, dp * rows, cols)

    return jax.shard_map(
        local_step,
        mesh=mesh,
        in_specs=(P(("rep", "dp"), None, None, "tp"), P("rep", "dp", "tp"), P("rep", "dp", "tp"), P("rep"), P()),
        out_specs=(P("rep", "dp", "tp"), P("rep", "dp", "tp"), P("rep", None, "tp")),
        check_vma=False,
    )
```

```python
import functools
import math

import jax
import jax.numpy as jnp
from jax import lax
from jax.experimental import pallas as pl
from jax.experimental.pallas import tpu as pltpu
from jax.sharding import PartitionSpec as P

MOMENTUM = 0.95
NS_STEPS = 5
COEF_A = 3.4445
COEF_B = -4.7750
COEF_C = 2.0315
NORM_EPS = 1e-7
MESH = pl.DeviceIdType.MESH
F32 = jnp.float32
BF16 = jnp.bfloat16
CHUNKS = 8
SLOTS = 6


def scoped(tag):
    def deco(fn):
        def inner(*args):
            with jax.named_scope(tag + "#a=" + "_".join(str(a) for a in args)):
                return fn(*args)
        return inner
    return deco


def make_plan(waves, stages):
    wire, lat, gather_wire, small = 1.41, 2.1, 2.81, 0.7
    step = (1.15, 1.15, 0.57, 0.6, 1.15, 1.15)
    now, link, ylink = 2.0, 0.0, 0.0
    waiting = []
    fresh = [(w, q) for w in range(waves) for q in range(CHUNKS)]
    rank = {"ring": 0, "gather": 1, "half": 2, "pair": 3}

    def run(event):
        nonlocal now, link, ylink
        kind, w, q = event[:3]
        now += 0.06
        if kind == "ring" and event[3] < stages:
            link = max(link, now) + wire
            waiting.append((link + lat, ("ring", w, q, event[3] + 1)))
        elif kind == "ring":
            link = max(link, now) + small
            waiting.append((link + lat + 0.5, ("gather", w, q)))
        elif kind == "gather":
            ylink = max(ylink, now) + gather_wire
            waiting.append((ylink + lat, ("half", w, q)))
        elif kind == "half":
            waiting.append((now + 1.7, ("pair", w, q)))

    def take(limit):
        due = [item for item in waiting if item[0] <= limit]
        if not due:
            return None
        best = min(due, key=lambda item: (item[1][1], rank[item[1][0]], item[0]))
        waiting.remove(best)
        return best[1]

    before, slots, after = [], {}, []
    todo = CHUNKS
    while todo:
        event = take(now)
        if event is None and fresh and link - now < 0.7:
            event = ("ring", *fresh.pop(0), 0)
        if event is None:
            times = [item[0] for item in waiting]
            if fresh:
                times.append(link - 0.69)
            now = max(now, min(times))
            continue
        run(event)
        before.append(event)
        todo -= event[0] == "pair" and event[1] == 0
    clock = now + 1.3
    for it in range(NS_STEPS):
        for slot in range(SLOTS if it < NS_STEPS - 1 else 4):
            clock += step[slot]
            now = clock
            found = []
            while True:
                event = take(now - 0.5)
                if event is None and fresh and link - now < 2.0:
                    event = ("ring", *fresh.pop(0), 0)
                if event is None:
                    break
                run(event)
                found.append(event)
            clock = now
            slots[it, slot] = found
    while fresh or waiting:
        if fresh:
            event = ("ring", *fresh.pop(0), 0)
        else:
            event = take(min(item[0] for item in waiting))
        run(event)
        after.append(event)
    return before, slots, after


def dot_nt(lhs, rhs):
    return lax.dot_general(lhs, rhs, (((1,), (1,)), ((), ())), preferred_element_type=F32)


def dot_nn(lhs, rhs):
    return jnp.dot(lhs, rhs, preferred_element_type=F32)


def muon_kernel(
    dims, grad, mom, wgt, rate, decay, momv, wgtv, full,
    gown, gpar, ring, usend, xs0, xs1, xs2, aown, apar, bmat, xfin, xback, sums,
    own_sem, mw_sem, gp_s, gp_r, ring_s, ring_r, a2a_s, a2a_r, yg_s, yg_r, half_s, half_r,
    xe_s, xe_r, ae_s, ae_r, bk_s, bk_r, ag_s, ag_r, ad_s, ad_r,
):
    nx, tp, mats, rows, cols = dims
    waves = mats // nx
    piece = rows // CHUNKS
    half = nx * rows
    width = tp * cols
    blk = min(256, half // 2)
    nblk = min(256, cols // 2)
    xs = (xs0, xs1)
    pong = xs2
    out_scale = 0.2 * math.sqrt(max(2 * half, width))

    d = lax.axis_index("dp")
    y = lax.axis_index("tp")
    x = d // 2
    c = d % 2
    turn = 1 - 2 * c
    nxt_x = (x + turn + nx) % nx
    partner = {"dp": 2 * x + (1 - c)}
    right = {"dp": 2 * nxt_x + c}

    my_cols = pl.ds(pl.multiple_of(y * cols, cols), cols)

    def at_x(dx):
        return {"dp": 2 * ((x + dx) % nx) + c}

    def at_y(dy):
        return {"tp": (y + dy) % tp}

    def remote(src, dst, send, recv, dev):
        return pltpu.make_async_remote_copy(
            src_ref=src, dst_ref=dst, send_sem=send, recv_sem=recv, device_id=dev, device_id_type=MESH
        )

    def wave(w):
        return pl.ds(w * nx, nx)

    def part(q):
        return pl.ds(q * piece, piece)

    def own_load(w, q):
        return pltpu.make_async_copy(
            grad.at[wave(w), :, c, part(q)], gown.at[wave(w), :, part(q)], own_sem.at[w, q]
        )

    def pair_copy(w, q):
        return remote(
            grad.at[wave(w), :, 1 - c, part(q)], gpar.at[wave(w), :, part(q)], gp_s.at[w, q], gp_r.at[w, q], partner
        )

    mom_load = pltpu.make_async_copy(mom, momv, mw_sem.at[0])
    wgt_load = pltpu.make_async_copy(wgt, wgtv, mw_sem.at[1])
    for w in range(waves):
        for q in range(CHUNKS):
            own_load(w, q).start()
    mom_load.start()
    wgt_load.start()

    barrier = pltpu.get_barrier_semaphore()
    peers = [partner] + [at_x(dx) for dx in range(1, nx)] + [at_y(dy) for dy in range(1, tp)]
    for peer in peers:
        pl.semaphore_signal(barrier, inc=1, device_id=peer, device_id_type=MESH)
    pl.semaphore_wait(barrier, len(peers))
    for w in range(waves):
        for q in range(CHUNKS):
            pair_copy(w, q).start()

    def ring_block(stage):
        return (x - turn * (1 + stage) + 4 * nx) % nx

    def ring_copy(w, q, stage):
        if stage == 0:
            src = gown.at[wave(w), ring_block(0), part(q)]
        else:
            src = ring.at[w, q, stage - 1]
        return remote(src, ring.at[w, q, stage], ring_s.at[w, q, stage], ring_r.at[w, q, stage], right)

    def a2a_copy(w, q, dx):
        owner = (x + dx) % nx
        return remote(
            usend.at[w * nx + owner, part(q)],
            xs[w].at[0, x, part(q), my_cols],
            a2a_s.at[w, q, dx], a2a_r.at[w, q, dx], at_x(dx),
        )

    def ring_event(w, q, stage):
        block = ring_block(stage)
        if stage == 0:
            own_load(w, q).wait()
            pair_copy(w, q).wait_recv()
        else:
            ring_copy(w, q, stage - 1).wait_recv()
        for i in range(nx):
            m = w * nx + i
            local = gown[m, block, part(q)] + gpar[m, block, part(q)]
            if stage == 0:
                gown[m, block, part(q)] = local
            elif stage < nx - 1:
                ring[w, q, stage - 1, i] = ring[w, q, stage - 1, i] + local
            else:
                grad_mean = (ring[w, q, stage - 1, i] + local) * (1.0 / (2 * nx))
                mom_new = MOMENTUM * momv[m, part(q)] + grad_mean
                momv[m, part(q)] = mom_new
                usend[m, part(q)] = (grad_mean + MOMENTUM * mom_new).astype(BF16)
        if stage < nx - 1:
            ring_copy(w, q, stage).start()
        else:
            for dx in (2, 1, 3):
                a2a_copy(w, q, dx).start()
            xs[w][0, x, part(q), my_cols] = usend[w * nx + x, part(q)]

    def gather_copy(w, q, dy):
        region = xs[w].at[0, :, part(q), my_cols]
        return remote(region, region, yg_s.at[w, q, dy - 1], yg_r.at[w, q, dy - 1], at_y(dy))

    def half_copy(w, q):
        return remote(
            xs[w].at[0, :, part(q)], xs[w].at[1, :, part(q)], half_s.at[w, q], half_r.at[w, q], partner
        )

    def gather_event(w, q):
        for dx in (1, 3, 2):
            a2a_copy(w, q, dx).wait_recv()
        for dy in (2, 1, 3):
            if dy < tp:
                gather_copy(w, q, dy).start()

    def add_squares(w, side, q):
        acc = sums[w]
        for i in range(nx):
            v = xs[w][side, i, part(q), :].astype(F32)
            v = v * v
            for n in range(width // 128):
                acc = acc + v[:, n * 128:(n + 1) * 128]
        sums[w] = acc

    def half_event(w, q):
        for dy in (1, 3, 2):
            if dy < tp:
                gather_copy(w, q, dy).wait_recv()
        half_copy(w, q).start()
        add_squares(w, 0, q)

    def pair_event(w, q):
        half_copy(w, q).wait_recv()
        add_squares(w, 1, q)

    @scoped("normalise")
    def normalise(w):
        for q in range(CHUNKS):
            half_copy(w, q).wait_send()
            for dy in range(1, tp):
                gather_copy(w, q, dy).wait_send()
        total = jnp.sum(sums[w])
        inv = 1.0 / (jnp.sqrt(jnp.full((8, 128), total, F32)) + NORM_EPS)
        inv = inv[0:1, 0:1]

        def scale_rows(r, carry):
            sl = pl.ds(pl.multiple_of(r * 16, 16), 16)
            for side in range(2):
                for i in range(nx):
                    xs[w][side, i, sl, :] = (xs[w][side, i, sl, :].astype(F32) * inv).astype(BF16)
            return carry

        lax.fori_loop(0, rows // 16, scale_rows, 0)

    own = pl.ds(0, half)
    own_blocks = half // blk
    n_chunks = width // nblk
    batch = max(1, n_chunks // 2)

    def chunk_copy(dst, par, n):
        col = pl.ds(pl.multiple_of(n * nblk, nblk), nblk)
        return remote(dst.at[0, :, :, col], dst.at[1, :, :, col], xe_s.at[par, n], xe_r.at[par, n], partner)

    def newton_schulz(w, service):
        def a_copy(par):
            return remote(aown.at[:, own], apar.at[par], ae_s.at[par], ae_r.at[par], partner)

        def a_block(cur, side, j):
            per = blk // rows if blk >= rows else 1
            rhs = cur[side, j * per:(j + 1) * per].reshape(blk, width)
            lhs = cur[0].reshape(half, width)
            col = (side * own_blocks + j) * blk
            aown[:, col:col + blk] = dot_nt(lhs, rhs).astype(BF16)

        def b_own(j):
            rs = slice(j * blk, (j + 1) * blk)
            sq = dot_nt(aown[...], aown[rs, :])
            bmat[:, rs] = (COEF_B * aown[:, rs].astype(F32) + COEF_C * sq).astype(BF16)

        def b_other(par, j):
            rs = slice(j * blk, (j + 1) * blk)
            ps = slice(half + j * blk, half + (j + 1) * blk)
            sq = dot_nn(aown[:, :half], aown[:, ps]) + dot_nn(aown[:, half:], apar[par, :, rs])
            bmat[:, ps] = (COEF_B * aown[:, ps].astype(F32) + COEF_C * sq).astype(BF16)

        def x_cols(cur, col):
            rhs = cur[:, :, :, col].reshape(2 * half, nblk)
            new = COEF_A * cur[0, :, :, col].reshape(half, nblk).astype(F32) + dot_nn(bmat[...], rhs)
            return new.astype(BF16)

        def iteration(it, par, cur, nxt, first, final):
            def drain_a():
                a_copy(1 - par).wait_send()

            def need_x():
                for n in range(n_chunks):
                    chunk_copy(cur, 1 - par, n).wait()

            def guarded(fn):
                if first is False:
                    fn()
                else:
                    pl.when(jnp.logical_not(first))(fn)

            guarded(drain_a)
            with jax.named_scope("a_own"):
                for j in range(own_blocks):
                    a_block(cur, 0, j)
            a_copy(par).start()
            service(it, 0)
            with jax.named_scope("x_wait"):
                guarded(need_x)
            with jax.named_scope("a_other"):
                for j in range(own_blocks):
                    a_block(cur, 1, j)
            service(it, 1)
            with jax.named_scope("b_own"):
                for j in range(own_blocks):
                    b_own(j)
            service(it, 2)
            with jax.named_scope("a_wait"):
                a_copy(par).wait_recv()
            with jax.named_scope("b_other"):
                for j in range(own_blocks):
                    b_other(par, j)
            service(it, 3)
            if final:
                with jax.named_scope("x_last"):
                    for n in range(cols // nblk):
                        col = pl.ds(pl.multiple_of(y * cols + n * nblk, nblk), nblk)
                        xfin[w, :, :, n * nblk:(n + 1) * nblk] = x_cols(cur, col).reshape(nx, rows, nblk)
            else:
                def x_pair(k, carry):
                    cols_of = [pl.ds(pl.multiple_of((2 * k + e) * nblk, nblk), nblk) for e in range(2)]
                    for col in cols_of:
                        nxt[0, :, :, col] = x_cols(cur, col).reshape(nx, rows, nblk)
                    for e in range(2):
                        chunk_copy(nxt, par, 2 * k + e).start()
                    return carry

                for part_no in range(2):
                    with jax.named_scope("x_step"):
                        lax.fori_loop(part_no * batch // 2, (part_no + 1) * batch // 2, x_pair, 0)
                    service(it, 4 + part_no)

        def pair_of_steps(p, carry):
            iteration((p, 0), 0, xs[w], pong, p == 0, False)
            iteration((p, 1), 1, pong, xs[w], False, False)
            return carry

        lax.fori_loop(0, NS_STEPS // 2, pair_of_steps, 0)
        iteration(NS_STEPS - 1, 0, xs[w], None, False, True)
        a_copy(0).wait_send()

    def back_copy(w, dx):
        return remote(
            xfin.at[w, (x + dx) % nx],
            xback.at[w * nx + x], bk_s.at[w, dx], bk_r.at[w, dx], at_x(dx),
        )

    def back_arrival(w, dx):
        m = w * nx + (x - dx + nx) % nx
        return remote(
            xfin.at[w, 0], xback.at[m], bk_s.at[w, dx], bk_r.at[w, dx], at_x(dx)
        )

    def back_send(w):
        for dx in (2, 1, 3):
            back_copy(w, dx).start()
        xback[w * nx + x] = xfin[w, x]

    order = (0, 1, 3, 2)

    def gather_slot(w, hop, j):
        holder = (x - turn * hop + 4 * nx) % nx
        return holder, w * nx + (holder - order[j] + nx) % nx

    def ag_copy(w, hop, j):
        holder, m = gather_slot(w, hop, j)
        block = full.at[m, holder, c]
        return remote(block, block, ag_s.at[m, hop], ag_r.at[m, hop], right)

    def ag_arrival(w, hop, j):
        holder, m = gather_slot(w, hop + 1, j)
        block = full.at[m, holder, c]
        return remote(block, block, ag_s.at[m, hop], ag_r.at[m, hop], right)

    def pair_full(w, hop, j):
        holder, m = gather_slot(w, hop, j)
        block = full.at[m, holder, c]
        return remote(block, block, ad_s.at[m, hop], ad_r.at[m, hop], partner)

    def pair_arrival(w, hop, j):
        holder = (x + turn * hop + 4 * nx) % nx
        m = w * nx + (holder - order[j] + nx) % nx
        block = full.at[m, holder, 1 - c]
        return remote(block, block, ad_s.at[m, hop], ad_r.at[m, hop], partner)

    def weight_event(w, j):
        dx = order[j]
        m = w * nx + (x - dx + nx) % nx
        if dx:
            back_arrival(w, dx).wait_recv()
        w_old = wgtv[m]
        w_new = w_old - rate[m] * (out_scale * xback[m].astype(F32) + decay[0] * w_old)
        wgtv[m] = w_new
        full[m, x, c] = w_new.astype(BF16)
        ag_copy(w, 0, j).start()
        pair_full(w, 0, j).start()

    def forward_event(w, hop, j):
        ag_arrival(w, hop - 1, j).wait_recv()
        if hop < nx - 1:
            ag_copy(w, hop, j).start()
        pair_full(w, hop, j).start()

    def finish_gather(w):
        for hop in range(nx):
            for j in range(nx):
                pair_arrival(w, hop, j).wait_recv()

    handlers = {"ring": ring_event, "gather": gather_event, "half": half_event, "pair": pair_event}

    def perform(events):
        for kind, *rest in events:
            with jax.named_scope(kind + "#a=" + "_".join(str(a) for a in rest)):
                handlers[kind](*rest)

    def server(table):
        def service(it, slot):
            if isinstance(it, tuple):
                p, odd = it
                for k in range(NS_STEPS // 2):
                    work = table.get((2 * k + odd, slot), [])
                    if work:
                        pl.when(p == k)(functools.partial(perform, work))
            else:
                perform(table.get((it, slot), []))
        return service

    handlers["weight"] = weight_event
    handlers["forward"] = forward_event
    before, during, after = make_plan(waves, nx - 1)
    for w in range(waves):
        sums[w] = jnp.zeros((piece, 128), F32)
    mom_load.wait()
    perform(before)
    normalise(0)
    newton_schulz(0, server(during))
    back_send(0)
    wgt_load.wait()
    perform([e for e in after if e[0] in ("ring", "gather")])
    perform([("weight", 0, 0)])
    perform([e for e in after if e[0] in ("half", "pair")])
    normalise(1)
    second = {
        (0, 4): [("weight", 0, 1)], (0, 5): [("weight", 0, 2)], (1, 0): [("weight", 0, 3)],
        (1, 2): [("forward", 0, 1, 0)], (1, 3): [("forward", 0, 1, 1)],
        (1, 4): [("forward", 0, 1, 2)], (1, 5): [("forward", 0, 1, 3)],
        (2, 2): [("forward", 0, 2, 0)], (2, 3): [("forward", 0, 2, 1)],
        (2, 4): [("forward", 0, 2, 2)], (2, 5): [("forward", 0, 2, 3)],
        (3, 2): [("forward", 0, 3, 0)], (3, 3): [("forward", 0, 3, 1)],
        (3, 4): [("forward", 0, 3, 2)], (3, 5): [("forward", 0, 3, 3)],
    }
    newton_schulz(1, server(second))
    back_send(1)
    perform([("weight", 1, j) for j in range(nx)])
    perform([("forward", 1, hop, j) for hop in range(1, nx) for j in range(nx)])
    with jax.named_scope("finish"):
        for w in range(waves):
            finish_gather(w)

    for w in range(waves):
        for q in range(CHUNKS):
            pair_copy(w, q).wait_send()
            for stage in range(nx - 1):
                ring_copy(w, q, stage).wait_send()
            for dx in range(1, nx):
                a2a_copy(w, q, dx).wait_send()
        for dx in range(1, nx):
            back_copy(w, dx).wait_send()
        for hop in range(nx):
            for j in range(nx):
                if hop < nx - 1:
                    ag_copy(w, hop, j).wait_send()
                pair_full(w, hop, j).wait_send()


def solution(mesh):
    dp = mesh.shape["dp"]
    tp = mesh.shape["tp"]
    nx = dp // 2

    def local_step(grad_local, mom_local, weight_local, learn_rate, decay_rate):
        mats, rows, cols = mom_local.shape
        waves = mats // nx
        piece = rows // CHUNKS
        half = nx * rows
        width = tp * cols
        n_chunks = width // min(256, cols // 2)
        dma = pltpu.SemaphoreType.DMA
        vmem = pltpu.VMEM
        anyspec = pl.BlockSpec(memory_space=pl.ANY)
        smem = pl.BlockSpec(memory_space=pltpu.SMEM)
        vspec = pl.BlockSpec(memory_space=pltpu.VMEM)
        grad_view = grad_local.reshape(mats, nx, 2, rows, cols)
        call = pl.pallas_call(
            functools.partial(muon_kernel, (nx, tp, mats, rows, cols)),
            out_shape=(
                vmem((mats, rows, cols), F32),
                vmem((mats, rows, cols), F32),
                vmem((mats, nx, 2, rows, cols), BF16),
            ),
            in_specs=[anyspec, anyspec, anyspec, smem, smem],
            out_specs=(vspec, vspec, vspec),
            scratch_shapes=[
                vmem((mats, nx, rows, cols), F32),
                vmem((mats, nx, rows, cols), F32),
                vmem((waves, CHUNKS, nx - 1, nx, piece, cols), F32),
                vmem((mats, rows, cols), BF16),
                vmem((2, nx, rows, width), BF16),
                vmem((2, nx, rows, width), BF16),
                vmem((2, nx, rows, width), BF16),
                vmem((half, 2 * half), BF16),
                vmem((2, half, half), BF16),
                vmem((half, 2 * half), BF16),
                vmem((waves, nx, rows, cols), BF16),
                vmem((mats, rows, cols), BF16),
                vmem((waves, piece, 128), F32),
                dma((waves, CHUNKS)),
                dma((2,)),
                dma((waves, CHUNKS)),
                dma((waves, CHUNKS)),
                dma((waves, CHUNKS, nx - 1)),
                dma((waves, CHUNKS, nx - 1)),
                dma((waves, CHUNKS, nx)),
                dma((waves, CHUNKS, nx)),
                dma((waves, CHUNKS, tp - 1)),
                dma((waves, CHUNKS, tp - 1)),
                dma((waves, CHUNKS)),
                dma((waves, CHUNKS)),
                dma((2, n_chunks)),
                dma((2, n_chunks)),
                dma((2,)),
                dma((2,)),
                dma((waves, nx)),
                dma((waves, nx)),
                dma((mats, nx)),
                dma((mats, nx)),
                dma((mats, nx)),
                dma((mats, nx)),
            ],
            compiler_params=pltpu.CompilerParams(
                collective_id=0, has_side_effects=True, vmem_limit_bytes=46 * 1024 * 1024
            ),
        )
        mom_new, weight_new, full = call(grad_view, mom_local, weight_local, learn_rate, decay_rate.reshape(1))
        return mom_new, weight_new, full.reshape(mats, dp * rows, cols)

    return jax.shard_map(
        local_step,
        mesh=mesh,
        in_specs=(P(("rep", "dp"), None, None, "tp"), P("rep", "dp", "tp"), P("rep", "dp", "tp"), P("rep"), P()),
        out_specs=(P("rep", "dp", "tp"), P("rep", "dp", "tp"), P("rep", None, "tp")),
        check_vma=False,
    )
```

```python
import functools
import math

import jax
import jax.numpy as jnp
from jax import lax
from jax.experimental import pallas as pl
from jax.experimental.pallas import tpu as pltpu
from jax.sharding import PartitionSpec as P

MOMENTUM = 0.95
NS_STEPS = 5
COEF_A = 3.4445
COEF_B = -4.7750
COEF_C = 2.0315
NORM_EPS = 1e-7
MESH = pl.DeviceIdType.MESH
F32 = jnp.float32
BF16 = jnp.bfloat16
CHUNKS = 8
SLOTS = 6


def scoped(tag):
    def deco(fn):
        def inner(*args):
            with jax.named_scope(tag + "#a=" + "_".join(str(a) for a in args)):
                return fn(*args)
        return inner
    return deco


def make_plan(waves, stages):
    wire, lat, gather_wire, small = 1.41, 2.0, 2.81, 0.7
    step = (1.4, 1.4, 0.8, 0.8, 1.68, 1.68)
    now, link, ylink = 2.0, 0.0, 0.0
    waiting = []
    fresh = [(w, q) for w in range(waves) for q in range(CHUNKS)]
    rank = {"ring": 0, "gather": 1, "half": 2, "pair": 3}

    def run(event):
        nonlocal now, link, ylink
        kind, w, q = event[:3]
        now += 0.06
        if kind == "ring" and event[3] < stages:
            link = max(link, now) + wire
            waiting.append((link + lat, ("ring", w, q, event[3] + 1)))
        elif kind == "ring":
            link = max(link, now) + small
            waiting.append((link + lat + 0.3, ("gather", w, q)))
        elif kind == "gather":
            ylink = max(ylink, now) + gather_wire
            waiting.append((ylink + lat, ("half", w, q)))
        elif kind == "half":
            waiting.append((now + 1.7, ("pair", w, q)))

    def take(limit):
        nonlocal now
        due = [item for item in waiting if item[0] <= limit]
        if not due:
            return None
        best = min(due, key=lambda item: (item[1][1], rank[item[1][0]], item[0]))
        waiting.remove(best)
        now = max(now, best[0])
        return best[1]

    before, slots, after = [], {}, []
    todo = CHUNKS
    while todo:
        event = take(now)
        usable = fresh and (fresh[0][0] == 0 or ("ring", 0, CHUNKS - 1, stages) in before)
        if event is None and usable and link - now < 0.7:
            event = ("ring", *fresh.pop(0), 0)
        if event is None:
            times = [item[0] for item in waiting]
            if usable:
                times.append(link - 0.69)
            now = max(now, min(times))
            continue
        run(event)
        before.append(event)
        todo -= event[0] == "pair" and event[1] == 0
    clock = now + 1.3
    for it in range(NS_STEPS):
        for slot in range(SLOTS if it < NS_STEPS - 1 else 4):
            clock += step[slot]
            now = clock
            found = []
            while True:
                event = take(now + 0.4)
                if event is None and fresh and link - now < 2.0:
                    event = ("ring", *fresh.pop(0), 0)
                if event is None:
                    break
                run(event)
                found.append(event)
            clock = now
            slots[it, slot] = found
    while fresh or waiting:
        if fresh:
            event = ("ring", *fresh.pop(0), 0)
        else:
            event = take(min(item[0] for item in waiting))
        run(event)
        after.append(event)
    return before, slots, after


def dot_nt(lhs, rhs):
    return lax.dot_general(lhs, rhs, (((1,), (1,)), ((), ())), preferred_element_type=F32)


def dot_nn(lhs, rhs):
    return jnp.dot(lhs, rhs, preferred_element_type=F32)


def muon_kernel(
    dims, grad, mom, wgt, rate, decay, momv, wgtv, full,
    gown, gpar, ring, usend, xs0, xs1, xs2, aown, apar, bmat, xfin, xback, sums,
    own_sem, mw_sem, gp_s, gp_r, ring_s, ring_r, a2a_s, a2a_r, yg_s, yg_r, half_s, half_r,
    xe_s, xe_r, ae_s, ae_r, bk_s, bk_r, ag_s, ag_r, ad_s, ad_r,
):
    nx, tp, mats, rows, cols = dims
    waves = mats // nx
    piece = rows // CHUNKS
    half = nx * rows
    width = tp * cols
    blk = min(256, half // 2)
    nblk = min(256, cols // 2)
    xs = (xs0, xs1)
    pong = xs2
    out_scale = 0.2 * math.sqrt(max(2 * half, width))

    d = lax.axis_index("dp")
    y = lax.axis_index("tp")
    x = d // 2
    c = d % 2
    turn = 1 - 2 * c
    nxt_x = (x + turn + nx) % nx
    partner = {"dp": 2 * x + (1 - c)}
    right = {"dp": 2 * nxt_x + c}

    my_cols = pl.ds(pl.multiple_of(y * cols, cols), cols)

    def at_x(dx):
        return {"dp": 2 * ((x + dx) % nx) + c}

    def at_y(dy):
        return {"tp": (y + dy) % tp}

    def remote(src, dst, send, recv, dev):
        return pltpu.make_async_remote_copy(
            src_ref=src, dst_ref=dst, send_sem=send, recv_sem=recv, device_id=dev, device_id_type=MESH
        )

    def all_of(like, sem):
        pltpu.make_async_copy(like, like, sem).wait()

    def wave(w):
        return pl.ds(w * nx, nx)

    def part(q):
        return pl.ds(q * piece, piece)

    def own_load(w, q):
        return pltpu.make_async_copy(
            grad.at[wave(w), :, c, part(q)], gown.at[wave(w), :, part(q)], own_sem.at[w, q]
        )

    def pair_copy(w, q):
        return remote(
            grad.at[wave(w), :, 1 - c, part(q)], gpar.at[wave(w), :, part(q)], gp_s.at[0], gp_r.at[w, q], partner
        )

    mom_load = pltpu.make_async_copy(mom, momv, mw_sem.at[0])
    wgt_load = pltpu.make_async_copy(wgt, wgtv, mw_sem.at[1])
    for w in range(waves):
        for q in range(CHUNKS):
            own_load(w, q).start()
    mom_load.start()
    wgt_load.start()

    barrier = pltpu.get_barrier_semaphore()
    peers = [partner] + [at_x(dx) for dx in range(1, nx)] + [at_y(dy) for dy in range(1, tp)]
    for peer in peers:
        pl.semaphore_signal(barrier, inc=1, device_id=peer, device_id_type=MESH)
    pl.semaphore_wait(barrier, len(peers))
    for w in range(waves):
        for q in range(CHUNKS):
            pair_copy(w, q).start()

    def ring_block(stage):
        return (x - turn * (1 + stage) + 4 * nx) % nx

    def ring_copy(w, q, stage):
        if stage == 0:
            src = gown.at[wave(w), ring_block(0), part(q)]
        else:
            src = ring.at[w, q, stage - 1]
        return remote(src, ring.at[w, q, stage], ring_s.at[0], ring_r.at[w, q, stage], right)

    def a2a_copy(w, q, dx):
        owner = (x + dx) % nx
        return remote(
            usend.at[w * nx + owner, part(q)],
            xs[w].at[0, x, part(q), my_cols],
            a2a_s.at[0], a2a_r.at[w, q], at_x(dx),
        )

    def ring_event(w, q, stage):
        block = ring_block(stage)
        if stage == 0:
            own_load(w, q).wait()
            pair_copy(w, q).wait_recv()
        else:
            ring_copy(w, q, stage - 1).wait_recv()
        for i in range(nx):
            m = w * nx + i
            local = gown[m, block, part(q)] + gpar[m, block, part(q)]
            if stage == 0:
                gown[m, block, part(q)] = local
            elif stage < nx - 1:
                ring[w, q, stage - 1, i] = ring[w, q, stage - 1, i] + local
            else:
                grad_mean = (ring[w, q, stage - 1, i] + local) * (1.0 / (2 * nx))
                mom_new = MOMENTUM * momv[m, part(q)] + grad_mean
                momv[m, part(q)] = mom_new
                usend[m, part(q)] = (grad_mean + MOMENTUM * mom_new).astype(BF16)
        if stage < nx - 1:
            ring_copy(w, q, stage).start()
        else:
            for dx in (2, 1, 3):
                a2a_copy(w, q, dx).start()
            xs[w][0, x, part(q), my_cols] = usend[w * nx + x, part(q)]

    def gather_copy(w, q, dy):
        region = xs[w].at[0, :, part(q), my_cols]
        return remote(region, region, yg_s.at[w], yg_r.at[w, q], at_y(dy))

    def half_copy(w, q):
        return remote(
            xs[w].at[0, :, part(q)], xs[w].at[1, :, part(q)], half_s.at[w], half_r.at[w, q], partner
        )

    def gather_event(w, q):
        all_of(usend.at[pl.ds(0, nx - 1), part(q)], a2a_r.at[w, q])
        for dy in (2, 1, 3):
            if dy < tp:
                gather_copy(w, q, dy).start()

    def add_squares(w, side, q):
        acc = sums[w]
        for i in range(nx):
            v = xs[w][side, i, part(q), :].astype(F32)
            v = v * v
            for n in range(width // 128):
                acc = acc + v[:, n * 128:(n + 1) * 128]
        sums[w] = acc

    def half_event(w, q):
        all_of(xs[w].at[0, :, part(q), pl.ds(0, width - cols)], yg_r.at[w, q])
        half_copy(w, q).start()
        add_squares(w, 0, q)

    def pair_event(w, q):
        half_copy(w, q).wait_recv()
        add_squares(w, 1, q)

    @scoped("normalise")
    def normalise(w):
        all_of(xs[w].at[0], half_s.at[w])
        all_of(xs[w].at[0, :, :, pl.ds(0, width - cols)], yg_s.at[w])
        total = jnp.sum(sums[w])
        inv = 1.0 / (jnp.sqrt(jnp.full((8, 128), total, F32)) + NORM_EPS)
        inv = inv[0:1, 0:1]

        def scale_rows(r, carry):
            sl = pl.ds(pl.multiple_of(r * 16, 16), 16)
            for side in range(2):
                for i in range(nx):
                    xs[w][side, i, sl, :] = (xs[w][side, i, sl, :].astype(F32) * inv).astype(BF16)
            return carry

        lax.fori_loop(0, rows // 16, scale_rows, 0)

    own = pl.ds(0, half)
    own_blocks = half // blk
    n_chunks = width // nblk
    batch = max(1, n_chunks // 2)

    def chunk_copy(dst, par, n):
        col = pl.ds(pl.multiple_of(n * nblk, nblk), nblk)
        return remote(dst.at[0, :, :, col], dst.at[1, :, :, col], xe_s.at[par], xe_r.at[par], partner)

    def newton_schulz(w, service):
        def a_copy(par):
            return remote(aown.at[:, own], apar.at[par], ae_s.at[par], ae_r.at[par], partner)

        def a_block(cur, side, j):
            per = blk // rows if blk >= rows else 1
            rhs = cur[side, j * per:(j + 1) * per].reshape(blk, width)
            lhs = cur[0].reshape(half, width)
            col = (side * own_blocks + j) * blk
            aown[:, col:col + blk] = dot_nt(lhs, rhs).astype(BF16)

        def b_own(j):
            rs = slice(j * blk, (j + 1) * blk)
            sq = dot_nt(aown[...], aown[rs, :])
            bmat[:, rs] = (COEF_B * aown[:, rs].astype(F32) + COEF_C * sq).astype(BF16)

        def b_other(par, j):
            rs = slice(j * blk, (j + 1) * blk)
            ps = slice(half + j * blk, half + (j + 1) * blk)
            sq = dot_nn(aown[:, :half], aown[:, ps]) + dot_nn(aown[:, half:], apar[par, :, rs])
            bmat[:, ps] = (COEF_B * aown[:, ps].astype(F32) + COEF_C * sq).astype(BF16)

        def x_cols(cur, col):
            rhs = cur[:, :, :, col].reshape(2 * half, nblk)
            new = COEF_A * cur[0, :, :, col].reshape(half, nblk).astype(F32) + dot_nn(bmat[...], rhs)
            return new.astype(BF16)

        def iteration(it, par, cur, nxt, first, final):
            def drain_a():
                a_copy(1 - par).wait_send()

            def need_x():
                all_of(cur.at[0], xe_s.at[1 - par])
                all_of(cur.at[1], xe_r.at[1 - par])

            def guarded(fn):
                if first is False:
                    fn()
                else:
                    pl.when(jnp.logical_not(first))(fn)

            guarded(drain_a)
            with jax.named_scope("a_own"):
                for j in range(own_blocks):
                    a_block(cur, 0, j)
            a_copy(par).start()
            service(it, 0)
            with jax.named_scope("x_wait"):
                guarded(need_x)
            with jax.named_scope("a_other"):
                for j in range(own_blocks):
                    a_block(cur, 1, j)
            service(it, 1)
            with jax.named_scope("b_own"):
                for j in range(own_blocks):
                    b_own(j)
            service(it, 2)
            with jax.named_scope("a_wait"):
                a_copy(par).wait_recv()
            with jax.named_scope("b_other"):
                for j in range(own_blocks):
                    b_other(par, j)
            service(it, 3)
            if final:
                with jax.named_scope("x_last"):
                    for n in range(cols // nblk):
                        col = pl.ds(pl.multiple_of(y * cols + n * nblk, nblk), nblk)
                        xfin[w, :, :, n * nblk:(n + 1) * nblk] = x_cols(cur, col).reshape(nx, rows, nblk)
            else:
                def x_pair(k, carry):
                    cols_of = [pl.ds(pl.multiple_of((2 * k + e) * nblk, nblk), nblk) for e in range(2)]
                    for col in cols_of:
                        nxt[0, :, :, col] = x_cols(cur, col).reshape(nx, rows, nblk)
                    for e in range(2):
                        chunk_copy(nxt, par, 2 * k + e).start()
                    return carry

                for part_no in range(2):
                    with jax.named_scope("x_step"):
                        lax.fori_loop(part_no * batch // 2, (part_no + 1) * batch // 2, x_pair, 0)
                    service(it, 4 + part_no)

        def pair_of_steps(p, carry):
            iteration((p, 0), 0, xs[w], pong, p == 0, False)
            iteration((p, 1), 1, pong, xs[w], False, False)
            return carry

        lax.fori_loop(0, NS_STEPS // 2, pair_of_steps, 0)
        iteration(NS_STEPS - 1, 0, xs[w], None, False, True)
        a_copy(0).wait_send()

    def back_copy(w, dx):
        return remote(
            xfin.at[w, (x + dx) % nx],
            xback.at[w * nx + x], bk_s.at[0], bk_r.at[w, dx], at_x(dx),
        )

    def back_arrival(w, dx):
        m = w * nx + (x - dx + nx) % nx
        return remote(
            xfin.at[w, 0], xback.at[m], bk_s.at[0], bk_r.at[w, dx], at_x(dx)
        )

    def back_send(w):
        for dx in (2, 1, 3):
            back_copy(w, dx).start()
        xback[w * nx + x] = xfin[w, x]

    order = (0, 1, 3, 2)

    def gather_slot(w, hop, j):
        holder = (x - turn * hop + 4 * nx) % nx
        return holder, w * nx + (holder - order[j] + nx) % nx

    def ag_copy(w, hop, j):
        holder, m = gather_slot(w, hop, j)
        block = full.at[m, holder, c]
        return remote(block, block, ag_s.at[0], ag_r.at[m, hop], right)

    def ag_arrival(w, hop, j):
        holder, m = gather_slot(w, hop + 1, j)
        block = full.at[m, holder, c]
        return remote(block, block, ag_s.at[0], ag_r.at[m, hop], right)

    def pair_full(w, hop, j):
        holder, m = gather_slot(w, hop, j)
        block = full.at[m, holder, c]
        return remote(block, block, ad_s.at[0], ad_r.at[w], partner)

    def weight_event(w, j):
        dx = order[j]
        m = w * nx + (x - dx + nx) % nx
        if dx:
            back_arrival(w, dx).wait_recv()
        w_old = wgtv[m]
        w_new = w_old - rate[m] * (out_scale * xback[m].astype(F32) + decay[0] * w_old)
        wgtv[m] = w_new
        full[m, x, c] = w_new.astype(BF16)
        ag_copy(w, 0, j).start()
        pair_full(w, 0, j).start()

    def forward_event(w, hop, j):
        ag_arrival(w, hop - 1, j).wait_recv()
        if hop < nx - 1:
            ag_copy(w, hop, j).start()
        pair_full(w, hop, j).start()

    def finish_gather(w):
        all_of(full.at[wave(w), :, 1 - c], ad_r.at[w])

    handlers = {"ring": ring_event, "gather": gather_event, "half": half_event, "pair": pair_event}

    def perform(events):
        for kind, *rest in events:
            with jax.named_scope(kind + "#a=" + "_".join(str(a) for a in rest)):
                handlers[kind](*rest)

    def server(table):
        def service(it, slot):
            if isinstance(it, tuple):
                p, odd = it
                for k in range(NS_STEPS // 2):
                    work = table.get((2 * k + odd, slot), [])
                    if work:
                        pl.when(p == k)(functools.partial(perform, work))
            else:
                perform(table.get((it, slot), []))
        return service

    handlers["weight"] = weight_event
    handlers["forward"] = forward_event
    before, during, after = make_plan(waves, nx - 1)
    for w in range(waves):
        sums[w] = jnp.zeros((piece, 128), F32)
    mom_load.wait()
    perform(before)
    normalise(0)
    newton_schulz(0, server(during))
    back_send(0)
    wgt_load.wait()
    perform([e for e in after if e[0] in ("ring", "gather")])
    perform([("weight", 0, 0)])
    perform([e for e in after if e[0] in ("half", "pair")])
    normalise(1)
    second = {
        (0, 4): [("weight", 0, 1)], (0, 5): [("weight", 0, 2)], (1, 0): [("weight", 0, 3)],
        (1, 2): [("forward", 0, 1, 0)], (1, 3): [("forward", 0, 1, 1)],
        (1, 4): [("forward", 0, 1, 2)], (1, 5): [("forward", 0, 1, 3)],
        (2, 2): [("forward", 0, 2, 0)], (2, 3): [("forward", 0, 2, 1)],
        (2, 4): [("forward", 0, 2, 2)], (2, 5): [("forward", 0, 2, 3)],
        (3, 2): [("forward", 0, 3, 0)], (3, 3): [("forward", 0, 3, 1)],
        (3, 4): [("forward", 0, 3, 2)], (3, 5): [("forward", 0, 3, 3)],
    }
    newton_schulz(1, server(second))
    back_send(1)
    perform([("weight", 1, j) for j in range(nx)])
    perform([("forward", 1, hop, j) for hop in range(1, nx) for j in range(nx)])
    with jax.named_scope("finish"):
        for w in range(waves):
            finish_gather(w)

    all_of(gpar, gp_s.at[0])
    all_of(ring, ring_s.at[0])
    all_of(usend.at[pl.ds(0, waves * (nx - 1))], a2a_s.at[0])
    all_of(xback.at[pl.ds(0, waves * (nx - 1))], bk_s.at[0])
    all_of(full.at[:, pl.ds(0, nx - 1), 0], ag_s.at[0])
    all_of(full.at[:, :, 0], ad_s.at[0])


def solution(mesh):
    dp = mesh.shape["dp"]
    tp = mesh.shape["tp"]
    nx = dp // 2

    def local_step(grad_local, mom_local, weight_local, learn_rate, decay_rate):
        mats, rows, cols = mom_local.shape
        waves = mats // nx
        piece = rows // CHUNKS
        half = nx * rows
        width = tp * cols
        n_chunks = width // min(256, cols // 2)
        dma = pltpu.SemaphoreType.DMA
        vmem = pltpu.VMEM
        anyspec = pl.BlockSpec(memory_space=pl.ANY)
        smem = pl.BlockSpec(memory_space=pltpu.SMEM)
        vspec = pl.BlockSpec(memory_space=pltpu.VMEM)
        grad_view = grad_local.reshape(mats, nx, 2, rows, cols)
        call = pl.pallas_call(
            functools.partial(muon_kernel, (nx, tp, mats, rows, cols)),
            out_shape=(
                vmem((mats, rows, cols), F32),
                vmem((mats, rows, cols), F32),
                vmem((mats, nx, 2, rows, cols), BF16),
            ),
            in_specs=[anyspec, anyspec, anyspec, smem, smem],
            out_specs=(vspec, vspec, vspec),
            scratch_shapes=[
                vmem((mats, nx, rows, cols), F32),
                vmem((mats, nx, rows, cols), F32),
                vmem((waves, CHUNKS, nx - 1, nx, piece, cols), F32),
                vmem((mats, rows, cols), BF16),
                vmem((2, nx, rows, width), BF16),
                vmem((2, nx, rows, width), BF16),
                vmem((2, nx, rows, width), BF16),
                vmem((half, 2 * half), BF16),
                vmem((2, half, half), BF16),
                vmem((half, 2 * half), BF16),
                vmem((waves, nx, rows, cols), BF16),
                vmem((mats, rows, cols), BF16),
                vmem((waves, piece, 128), F32),
                dma((waves, CHUNKS)),
                dma((2,)),
                dma((1,)),
                dma((waves, CHUNKS)),
                dma((1,)),
                dma((waves, CHUNKS, nx - 1)),
                dma((1,)),
                dma((waves, CHUNKS)),
                dma((waves,)),
                dma((waves, CHUNKS)),
                dma((waves,)),
                dma((waves, CHUNKS)),
                dma((2,)),
                dma((2,)),
                dma((2,)),
                dma((2,)),
                dma((1,)),
                dma((waves, nx)),
                dma((1,)),
                dma((mats, nx - 1)),
                dma((1,)),
                dma((waves,)),
            ],
            compiler_params=pltpu.CompilerParams(
                collective_id=0, has_side_effects=True, vmem_limit_bytes=46 * 1024 * 1024
            ),
        )
        mom_new, weight_new, full = call(grad_view, mom_local, weight_local, learn_rate, decay_rate.reshape(1))
        return mom_new, weight_new, full.reshape(mats, dp * rows, cols)

    return jax.shard_map(
        local_step,
        mesh=mesh,
        in_specs=(P(("rep", "dp"), None, None, "tp"), P("rep", "dp", "tp"), P("rep", "dp", "tp"), P("rep"), P()),
        out_specs=(P("rep", "dp", "tp"), P("rep", "dp", "tp"), P("rep", None, "tp")),
        check_vma=False,
    )
```

```python
import functools
import math

import jax
import jax.numpy as jnp
from jax import lax
from jax.experimental import pallas as pl
from jax.experimental.pallas import tpu as pltpu
from jax.sharding import PartitionSpec as P

MOMENTUM = 0.95
NS_STEPS = 5
COEF_A = 3.4445
COEF_B = -4.7750
COEF_C = 2.0315
NORM_EPS = 1e-7
MESH = pl.DeviceIdType.MESH
F32 = jnp.float32
BF16 = jnp.bfloat16
CHUNKS = 8
SLOTS = 6


def scoped(tag):
    def deco(fn):
        def inner(*args):
            with jax.named_scope(tag + "#a=" + "_".join(str(a) for a in args)):
                return fn(*args)
        return inner
    return deco


def make_plan(waves, stages):
    wire, lat, gather_wire, small = 1.41, 2.4, 2.81, 0.7
    step = (1.4, 1.4, 1.5, 0.05, 1.68, 1.68)
    now, link, ylink = 2.0, 0.0, 0.0
    waiting = []
    fresh = [(w, q) for w in range(waves) for q in range(CHUNKS)]
    rank = {"ring": 0, "gather": 1, "half": 2, "pair": 3}

    def run(event):
        nonlocal now, link, ylink
        kind, w, q = event[:3]
        now += 0.06
        if kind == "ring" and event[3] < stages:
            link = max(link, now) + wire
            waiting.append((link + lat, ("ring", w, q, event[3] + 1)))
        elif kind == "ring":
            link = max(link, now) + small
            waiting.append((link + lat + 0.3, ("gather", w, q)))
        elif kind == "gather":
            ylink = max(ylink, now) + gather_wire
            waiting.append((ylink + lat, ("half", w, q)))
        elif kind == "half":
            waiting.append((now + 1.7, ("pair", w, q)))

    def take(limit):
        nonlocal now
        due = [item for item in waiting if item[0] <= limit]
        if not due:
            return None
        best = min(due, key=lambda item: (item[1][1], rank[item[1][0]], item[0]))
        waiting.remove(best)
        now = max(now, best[0])
        return best[1]

    before, slots, after = [], {}, []
    todo = CHUNKS
    while todo:
        event = take(now)
        usable, depth = False, 2.0
        if fresh and fresh[0][0]:
            started = len([e for e in before if e[1] and e[0] == "ring" and not e[3]])
            usable = ("ring", 0, CHUNKS - 1, stages - 1) in before and started < 1
            usable = usable or ("ring", 0, CHUNKS - 1, stages) in before
        elif fresh:
            usable = True
        if event is None and usable and link - now < depth:
            event = ("ring", *fresh.pop(0), 0)
        if event is None:
            times = [item[0] for item in waiting]
            if usable:
                times.append(link - depth + 0.01)
            now = max(now, min(times))
            continue
        run(event)
        before.append(event)
        todo -= event[0] == "pair" and event[1] == 0
    clock = now + 1.3
    for it in range(NS_STEPS):
        for slot in range(SLOTS if it < NS_STEPS - 1 else 4):
            clock += step[slot]
            now = clock
            found = []
            while True:
                event = take(now + 0.2)
                if event is None and fresh and link - now < 2.0:
                    event = ("ring", *fresh.pop(0), 0)
                if event is None:
                    break
                run(event)
                found.append(event)
            clock = now
            slots[it, slot] = found
    while fresh or waiting:
        if fresh:
            event = ("ring", *fresh.pop(0), 0)
        else:
            event = take(min(item[0] for item in waiting))
        run(event)
        after.append(event)
    return before, slots, after


def dot_nt(lhs, rhs):
    return lax.dot_general(lhs, rhs, (((1,), (1,)), ((), ())), preferred_element_type=F32)


def dot_nn(lhs, rhs):
    return jnp.dot(lhs, rhs, preferred_element_type=F32)


def muon_kernel(
    dims, grad, mom, wgt, rate, decay, momv, wgtv, full,
    gown, gpar, ring, usend, xs0, xs1, xs2, aown, apar, bmat, xfin, xback, sums,
    own_sem, mw_sem, gp_s, gp_r, ring_s, ring_r, a2a_s, a2a_r, yg_s, yg_r, half_s, half_r,
    xe_s, xe_r, ae_s, ae_r, bk_s, bk_r, ag_s, ag_r, ad_s, ad_r,
):
    nx, tp, mats, rows, cols = dims
    waves = mats // nx
    piece = rows // CHUNKS
    half = nx * rows
    width = tp * cols
    blk = min(256, half // 2)
    nblk = min(256, cols // 2)
    xs = (xs0, xs1)
    pong = xs2
    out_scale = 0.2 * math.sqrt(max(2 * half, width))

    d = lax.axis_index("dp")
    y = lax.axis_index("tp")
    x = d // 2
    c = d % 2
    turn = 1 - 2 * c
    nxt_x = (x + turn + nx) % nx
    partner = {"dp": 2 * x + (1 - c)}
    right = {"dp": 2 * nxt_x + c}

    my_cols = pl.ds(pl.multiple_of(y * cols, cols), cols)

    def at_x(dx):
        return {"dp": 2 * ((x + dx) % nx) + c}

    def at_y(dy):
        return {"tp": (y + dy) % tp}

    def remote(src, dst, send, recv, dev):
        return pltpu.make_async_remote_copy(
            src_ref=src, dst_ref=dst, send_sem=send, recv_sem=recv, device_id=dev, device_id_type=MESH
        )

    def all_of(like, sem):
        pltpu.make_async_copy(like, like, sem).wait()

    def wave(w):
        return pl.ds(w * nx, nx)

    def part(q):
        return pl.ds(q * piece, piece)

    def own_load(w, q):
        return pltpu.make_async_copy(
            grad.at[wave(w), :, c, part(q)], gown.at[wave(w), :, part(q)], own_sem.at[w, q]
        )

    def pair_copy(w, q):
        return remote(
            grad.at[wave(w), :, 1 - c, part(q)], gpar.at[wave(w), :, part(q)], gp_s.at[0], gp_r.at[w, q], partner
        )

    mom_load = pltpu.make_async_copy(mom, momv, mw_sem.at[0])
    wgt_load = pltpu.make_async_copy(wgt, wgtv, mw_sem.at[1])
    for w in range(waves):
        for q in range(CHUNKS):
            own_load(w, q).start()
    mom_load.start()
    wgt_load.start()

    barrier = pltpu.get_barrier_semaphore()
    peers = [partner] + [at_x(dx) for dx in range(1, nx)] + [at_y(dy) for dy in range(1, tp)]
    for peer in peers:
        pl.semaphore_signal(barrier, inc=1, device_id=peer, device_id_type=MESH)
    pl.semaphore_wait(barrier, len(peers))
    for w in range(waves):
        for q in range(CHUNKS):
            pair_copy(w, q).start()

    def ring_block(stage):
        return (x - turn * (1 + stage) + 4 * nx) % nx

    def ring_copy(w, q, stage):
        if stage == 0:
            src = gown.at[wave(w), ring_block(0), part(q)]
        else:
            src = ring.at[w, q, stage - 1]
        return remote(src, ring.at[w, q, stage], ring_s.at[0], ring_r.at[w, q, stage], right)

    def a2a_copy(w, q, dx):
        owner = (x + dx) % nx
        return remote(
            usend.at[w * nx + owner, part(q)],
            xs[w].at[0, x, part(q), my_cols],
            a2a_s.at[0], a2a_r.at[w, q], at_x(dx),
        )

    def ring_event(w, q, stage):
        block = ring_block(stage)
        if stage == 0:
            own_load(w, q).wait()
            pair_copy(w, q).wait_recv()
        else:
            ring_copy(w, q, stage - 1).wait_recv()
        for i in range(nx):
            m = w * nx + i
            local = gown[m, block, part(q)] + gpar[m, block, part(q)]
            if stage == 0:
                gown[m, block, part(q)] = local
            elif stage < nx - 1:
                ring[w, q, stage - 1, i] = ring[w, q, stage - 1, i] + local
            else:
                grad_mean = (ring[w, q, stage - 1, i] + local) * (1.0 / (2 * nx))
                mom_new = MOMENTUM * momv[m, part(q)] + grad_mean
                momv[m, part(q)] = mom_new
                usend[m, part(q)] = (grad_mean + MOMENTUM * mom_new).astype(BF16)
        if stage < nx - 1:
            ring_copy(w, q, stage).start()
        else:
            for dx in (2, 1, 3):
                a2a_copy(w, q, dx).start()
            xs[w][0, x, part(q), my_cols] = usend[w * nx + x, part(q)]

    def gather_copy(w, q, dy):
        region = xs[w].at[0, :, part(q), my_cols]
        return remote(region, region, yg_s.at[w], yg_r.at[w, q], at_y(dy))

    def half_copy(w, q):
        return remote(
            xs[w].at[0, :, part(q)], xs[w].at[1, :, part(q)], half_s.at[w], half_r.at[w, q], partner
        )

    def gather_event(w, q):
        all_of(usend.at[pl.ds(0, nx - 1), part(q)], a2a_r.at[w, q])
        for dy in (2, 1, 3):
            if dy < tp:
                gather_copy(w, q, dy).start()

    def add_squares(w, side, q):
        acc = sums[w]
        for i in range(nx):
            v = xs[w][side, i, part(q), :].astype(F32)
            v = v * v
            for n in range(width // 128):
                acc = acc + v[:, n * 128:(n + 1) * 128]
        sums[w] = acc

    def half_event(w, q):
        all_of(xs[w].at[0, :, part(q), pl.ds(0, width - cols)], yg_r.at[w, q])
        half_copy(w, q).start()
        add_squares(w, 0, q)

    def pair_event(w, q):
        half_copy(w, q).wait_recv()
        add_squares(w, 1, q)

    @scoped("normalise")
    def normalise(w):
        all_of(xs[w].at[0], half_s.at[w])
        all_of(xs[w].at[0, :, :, pl.ds(0, width - cols)], yg_s.at[w])
        total = jnp.sum(sums[w])
        inv = 1.0 / (jnp.sqrt(jnp.full((8, 128), total, F32)) + NORM_EPS)
        inv = inv[0:1, 0:1]

        def scale_rows(r, carry):
            sl = pl.ds(pl.multiple_of(r * 16, 16), 16)
            for side in range(2):
                for i in range(nx):
                    xs[w][side, i, sl, :] = (xs[w][side, i, sl, :].astype(F32) * inv).astype(BF16)
            return carry

        lax.fori_loop(0, rows // 16, scale_rows, 0)

    own = pl.ds(0, half)
    own_blocks = half // blk
    n_chunks = width // nblk
    batch = max(1, n_chunks // 2)

    def chunk_copy(dst, par, n):
        col = pl.ds(pl.multiple_of(n * nblk, nblk), nblk)
        return remote(dst.at[0, :, :, col], dst.at[1, :, :, col], xe_s.at[par], xe_r.at[par], partner)

    def newton_schulz(w, service):
        def a_copy(par):
            slot = (par + w) % 2
            return remote(aown.at[:, own], apar.at[slot], ae_s.at[slot], ae_r.at[slot], partner)

        def a_block(cur, side, j):
            per = blk // rows if blk >= rows else 1
            rhs = cur[side, j * per:(j + 1) * per].reshape(blk, width)
            lhs = cur[0].reshape(half, width)
            col = (side * own_blocks + j) * blk
            aown[:, col:col + blk] = dot_nt(lhs, rhs).astype(BF16)

        def b_own(j):
            rs = slice(j * blk, (j + 1) * blk)
            sq = dot_nt(aown[...], aown[rs, :])
            bmat[:, rs] = (COEF_B * aown[:, rs].astype(F32) + COEF_C * sq).astype(BF16)

        def b_other(par, j):
            rs = slice(j * blk, (j + 1) * blk)
            ps = slice(half + j * blk, half + (j + 1) * blk)
            sq = dot_nn(aown[:, :half], aown[:, ps]) + dot_nn(aown[:, half:], apar[(par + w) % 2, :, rs])
            bmat[:, ps] = (COEF_B * aown[:, ps].astype(F32) + COEF_C * sq).astype(BF16)

        def x_cols(cur, col):
            rhs = cur[:, :, :, col].reshape(2 * half, nblk)
            new = COEF_A * cur[0, :, :, col].reshape(half, nblk).astype(F32) + dot_nn(bmat[...], rhs)
            return new.astype(BF16)

        def iteration(it, par, cur, nxt, first, final):
            def drain_a():
                a_copy(1 - par).wait_send()

            def need_x():
                all_of(cur.at[0], xe_s.at[1 - par])
                all_of(cur.at[1], xe_r.at[1 - par])

            def guarded(fn):
                if first is False:
                    fn()
                else:
                    pl.when(jnp.logical_not(first))(fn)

            guarded(drain_a)
            with jax.named_scope("a_own"):
                for j in range(own_blocks):
                    a_block(cur, 0, j)
            a_copy(par).start()
            service(it, 0)
            with jax.named_scope("x_wait"):
                guarded(need_x)
            with jax.named_scope("a_other"):
                for j in range(own_blocks):
                    a_block(cur, 1, j)
            service(it, 1)
            with jax.named_scope("a_wait"):
                a_copy(par).wait_recv()
            with jax.named_scope("b_step"):
                for j in range(own_blocks):
                    b_own(j)
                for j in range(own_blocks):
                    b_other(par, j)
            service(it, 2)
            service(it, 3)
            if final:
                with jax.named_scope("x_last"):
                    for n in range(cols // nblk):
                        col = pl.ds(pl.multiple_of(y * cols + n * nblk, nblk), nblk)
                        xfin[w, :, :, n * nblk:(n + 1) * nblk] = x_cols(cur, col).reshape(nx, rows, nblk)
            else:
                def x_pair(k, carry):
                    cols_of = [pl.ds(pl.multiple_of((2 * k + e) * nblk, nblk), nblk) for e in range(2)]
                    for col in cols_of:
                        nxt[0, :, :, col] = x_cols(cur, col).reshape(nx, rows, nblk)
                    for e in range(2):
                        chunk_copy(nxt, par, 2 * k + e).start()
                    return carry

                for part_no in range(2):
                    with jax.named_scope("x_step"):
                        lax.fori_loop(part_no * batch // 2, (part_no + 1) * batch // 2, x_pair, 0)
                    service(it, 4 + part_no)

        def pair_of_steps(p, carry):
            iteration((p, 0), 0, xs[w], pong, p == 0, False)
            iteration((p, 1), 1, pong, xs[w], False, False)
            return carry

        lax.fori_loop(0, NS_STEPS // 2, pair_of_steps, 0)
        iteration(NS_STEPS - 1, 0, xs[w], None, False, True)
        a_copy(0).wait_send()

    def back_copy(w, dx):
        return remote(
            xfin.at[w, (x + dx) % nx],
            xback.at[w * nx + x], bk_s.at[0], bk_r.at[w, dx], at_x(dx),
        )

    def back_arrival(w, dx):
        m = w * nx + (x - dx + nx) % nx
        return remote(
            xfin.at[w, 0], xback.at[m], bk_s.at[0], bk_r.at[w, dx], at_x(dx)
        )

    def back_send(w):
        for dx in (2, 1, 3):
            back_copy(w, dx).start()
        xback[w * nx + x] = xfin[w, x]

    order = (0, 1, 3, 2)

    def gather_slot(w, hop, j):
        holder = (x - turn * hop + 4 * nx) % nx
        return holder, w * nx + (holder - order[j] + nx) % nx

    def ag_copy(w, hop, j):
        holder, m = gather_slot(w, hop, j)
        block = full.at[m, holder, c]
        return remote(block, block, ag_s.at[0], ag_r.at[m, hop], right)

    def ag_arrival(w, hop, j):
        holder, m = gather_slot(w, hop + 1, j)
        block = full.at[m, holder, c]
        return remote(block, block, ag_s.at[0], ag_r.at[m, hop], right)

    def pair_full(w, hop, j):
        holder, m = gather_slot(w, hop, j)
        block = full.at[m, holder, c]
        return remote(block, block, ad_s.at[0], ad_r.at[w], partner)

    def weight_event(w, j):
        dx = order[j]
        m = w * nx + (x - dx + nx) % nx
        if dx:
            back_arrival(w, dx).wait_recv()
        w_old = wgtv[m]
        w_new = w_old - rate[m] * (out_scale * xback[m].astype(F32) + decay[0] * w_old)
        wgtv[m] = w_new
        full[m, x, c] = w_new.astype(BF16)
        ag_copy(w, 0, j).start()
        pair_full(w, 0, j).start()

    def forward_event(w, hop, j):
        ag_arrival(w, hop - 1, j).wait_recv()
        if hop < nx - 1:
            ag_copy(w, hop, j).start()
        pair_full(w, hop, j).start()

    def finish_gather(w):
        all_of(full.at[wave(w), :, 1 - c], ad_r.at[w])

    handlers = {"ring": ring_event, "gather": gather_event, "half": half_event, "pair": pair_event}

    def perform(events):
        for kind, *rest in events:
            with jax.named_scope(kind + "#a=" + "_".join(str(a) for a in rest)):
                handlers[kind](*rest)

    def server(table):
        def service(it, slot):
            if isinstance(it, tuple):
                p, odd = it
                for k in range(NS_STEPS // 2):
                    work = table.get((2 * k + odd, slot), [])
                    if work:
                        pl.when(p == k)(functools.partial(perform, work))
            else:
                perform(table.get((it, slot), []))
        return service

    handlers["weight"] = weight_event
    handlers["forward"] = forward_event
    before, during, after = make_plan(waves, nx - 1)
    for w in range(waves):
        sums[w] = jnp.zeros((piece, 128), F32)
    mom_load.wait()
    perform(before)
    normalise(0)
    newton_schulz(0, server(during))
    back_send(0)
    wgt_load.wait()
    perform([e for e in after if e[0] in ("ring", "gather")])
    perform([("weight", 0, 0)])
    perform([e for e in after if e[0] in ("half", "pair")])
    normalise(1)
    second = {
        (0, 4): [("weight", 0, 1)], (0, 5): [("weight", 0, 2)], (1, 0): [("weight", 0, 3)],
        (1, 2): [("forward", 0, 1, 0)], (1, 3): [("forward", 0, 1, 1)],
        (1, 4): [("forward", 0, 1, 2)], (1, 5): [("forward", 0, 1, 3)],
        (2, 2): [("forward", 0, 2, 0)], (2, 3): [("forward", 0, 2, 1)],
        (2, 4): [("forward", 0, 2, 2)], (2, 5): [("forward", 0, 2, 3)],
        (3, 2): [("forward", 0, 3, 0)], (3, 3): [("forward", 0, 3, 1)],
        (3, 4): [("forward", 0, 3, 2)], (3, 5): [("forward", 0, 3, 3)],
    }
    newton_schulz(1, server(second))
    back_send(1)
    perform([("weight", 1, j) for j in range(nx)])
    perform([("forward", 1, hop, j) for hop in range(1, nx) for j in range(nx)])
    with jax.named_scope("finish"):
        for w in range(waves):
            finish_gather(w)

    all_of(gpar, gp_s.at[0])
    all_of(ring, ring_s.at[0])
    all_of(usend.at[pl.ds(0, waves * (nx - 1))], a2a_s.at[0])
    all_of(xback.at[pl.ds(0, waves * (nx - 1))], bk_s.at[0])
    all_of(full.at[:, pl.ds(0, nx - 1), 0], ag_s.at[0])
    all_of(full.at[:, :, 0], ad_s.at[0])


def store_kernel(a, b, c, a_out, b_out, c_out, sem):
    copies = [
        pltpu.make_async_copy(src, dst, sem.at[i])
        for i, (src, dst) in enumerate(((c, c_out), (b, b_out), (a, a_out)))
    ]
    for copy in copies:
        copy.start()
    for copy in copies:
        copy.wait()


def solution(mesh):
    dp = mesh.shape["dp"]
    tp = mesh.shape["tp"]
    nx = dp // 2

    def local_step(grad_local, mom_local, weight_local, learn_rate, decay_rate):
        mats, rows, cols = mom_local.shape
        waves = mats // nx
        piece = rows // CHUNKS
        half = nx * rows
        width = tp * cols
        n_chunks = width // min(256, cols // 2)
        dma = pltpu.SemaphoreType.DMA
        vmem = pltpu.VMEM
        anyspec = pl.BlockSpec(memory_space=pl.ANY)
        smem = pl.BlockSpec(memory_space=pltpu.SMEM)
        vspec = pl.BlockSpec(memory_space=pltpu.VMEM)
        grad_view = grad_local.reshape(mats, nx, 2, rows, cols)
        call = pl.pallas_call(
            functools.partial(muon_kernel, (nx, tp, mats, rows, cols)),
            out_shape=(
                vmem((mats, rows, cols), F32),
                vmem((mats, rows, cols), F32),
                vmem((mats, nx, 2, rows, cols), BF16),
            ),
            in_specs=[anyspec, anyspec, anyspec, smem, smem],
            out_specs=(vspec, vspec, vspec),
            scratch_shapes=[
                vmem((mats, nx, rows, cols), F32),
                vmem((mats, nx, rows, cols), F32),
                vmem((waves, CHUNKS, nx - 1, nx, piece, cols), F32),
                vmem((mats, rows, cols), BF16),
                vmem((2, nx, rows, width), BF16),
                vmem((2, nx, rows, width), BF16),
                vmem((2, nx, rows, width), BF16),
                vmem((half, 2 * half), BF16),
                vmem((2, half, half), BF16),
                vmem((half, 2 * half), BF16),
                vmem((waves, nx, rows, cols), BF16),
                vmem((mats, rows, cols), BF16),
                vmem((waves, piece, 128), F32),
                dma((waves, CHUNKS)),
                dma((2,)),
                dma((1,)),
                dma((waves, CHUNKS)),
                dma((1,)),
                dma((waves, CHUNKS, nx - 1)),
                dma((1,)),
                dma((waves, CHUNKS)),
                dma((waves,)),
                dma((waves, CHUNKS)),
                dma((waves,)),
                dma((waves, CHUNKS)),
                dma((2,)),
                dma((2,)),
                dma((2,)),
                dma((2,)),
                dma((1,)),
                dma((waves, nx)),
                dma((1,)),
                dma((mats, nx - 1)),
                dma((1,)),
                dma((waves,)),
            ],
            compiler_params=pltpu.CompilerParams(
                collective_id=0, has_side_effects=True, vmem_limit_bytes=46 * 1024 * 1024
            ),
        )
        results = call(grad_view, mom_local, weight_local, learn_rate, decay_rate.reshape(1))
        results = [pltpu.with_memory_space_constraint(r, pltpu.VMEM) for r in results]
        mom_new, weight_new, full = pl.pallas_call(
            store_kernel,
            out_shape=tuple(jax.ShapeDtypeStruct(r.shape, r.dtype) for r in results),
            in_specs=[vspec] * 3,
            out_specs=(anyspec,) * 3,
            scratch_shapes=[dma((3,))],
            compiler_params=pltpu.CompilerParams(vmem_limit_bytes=1024 * 1024),
        )(*results)
        return mom_new, weight_new, full.reshape(mats, dp * rows, cols)

    return jax.shard_map(
        local_step,
        mesh=mesh,
        in_specs=(P(("rep", "dp"), None, None, "tp"), P("rep", "dp", "tp"), P("rep", "dp", "tp"), P("rep"), P()),
        out_specs=(P("rep", "dp", "tp"), P("rep", "dp", "tp"), P("rep", None, "tp")),
        check_vma=False,
    )
```

```python
import functools
import math

import jax
import jax.numpy as jnp
from jax import lax
from jax.experimental import pallas as pl
from jax.experimental.pallas import tpu as pltpu
from jax.sharding import PartitionSpec as P

MOMENTUM = 0.95
NS_STEPS = 5
COEF_A = 3.4445
COEF_B = -4.7750
COEF_C = 2.0315
NORM_EPS = 1e-7
MESH = pl.DeviceIdType.MESH
F32 = jnp.float32
BF16 = jnp.bfloat16
CHUNKS = 8
SLOTS = 6


def scoped(tag):
    def deco(fn):
        def inner(*args):
            with jax.named_scope(tag + "#a=" + "_".join(str(a) for a in args)):
                return fn(*args)
        return inner
    return deco


def make_plan(waves, stages):
    wire, lat, gather_wire, small = 1.41, 2.0, 2.81, 0.7
    step = (1.4, 1.4, 1.5, 0.05, 1.68, 1.68)
    now, link, ylink = 2.0, 0.0, 0.0
    waiting = []
    fresh = [(w, q) for w in range(waves) for q in range(CHUNKS)]
    rank = {"ring": 0, "gather": 1, "half": 2, "pair": 3}

    def run(event):
        nonlocal now, link, ylink
        kind, w, q = event[:3]
        now += 0.06
        if kind == "ring" and event[3] < stages:
            link = max(link, now) + wire
            waiting.append((link + lat, ("ring", w, q, event[3] + 1)))
        elif kind == "ring":
            link = max(link, now) + small
            waiting.append((link + lat + 0.3, ("gather", w, q)))
        elif kind == "gather":
            ylink = max(ylink, now) + gather_wire
            waiting.append((ylink + lat, ("half", w, q)))
        elif kind == "half":
            waiting.append((now + 1.7, ("pair", w, q)))

    def take(limit, late=0.0):
        nonlocal now
        due = [item for item in waiting if item[0] <= limit - late * item[1][1]]
        if not due:
            return None
        best = min(due, key=lambda item: (item[1][1], rank[item[1][0]], item[0]))
        waiting.remove(best)
        now = max(now, best[0])
        return best[1]

    before, slots, after = [], {}, []
    todo = CHUNKS
    while todo:
        event = take(now, 1.5)
        usable, depth = False, 1.2
        if fresh and fresh[0][0]:
            started = len([e for e in before if e[1] and e[0] == "ring" and not e[3]])
            usable = ("ring", 0, CHUNKS - 1, stages - 1) in before and started < 1
            usable = usable or ("ring", 0, CHUNKS - 1, stages) in before
        elif fresh:
            usable = True
        if event is None and usable and link - now < depth:
            event = ("ring", *fresh.pop(0), 0)
        if event is None:
            times = [item[0] + 1.5 * item[1][1] for item in waiting]
            if usable:
                times.append(link - depth + 0.01)
            now = max(now + 0.01, min(times))
            continue
        run(event)
        before.append(event)
        todo -= event[0] == "pair" and event[1] == 0
    clock = now + 1.3
    for it in range(NS_STEPS):
        for slot in range(SLOTS if it < NS_STEPS - 1 else 4):
            clock += step[slot]
            now = clock
            found = []
            while True:
                event = take(now + 0.2)
                if event is None and fresh and link - now < 2.0:
                    event = ("ring", *fresh.pop(0), 0)
                if event is None:
                    break
                run(event)
                found.append(event)
            clock = now
            slots[it, slot] = found
    while fresh or waiting:
        if fresh:
            event = ("ring", *fresh.pop(0), 0)
        else:
            event = take(min(item[0] for item in waiting))
        run(event)
        after.append(event)
    return before, slots, after


def dot_nt(lhs, rhs):
    return lax.dot_general(lhs, rhs, (((1,), (1,)), ((), ())), preferred_element_type=F32)


def dot_nn(lhs, rhs):
    return jnp.dot(lhs, rhs, preferred_element_type=F32)


def muon_kernel(
    dims, grad, mom, wgt, rate, decay, momv, wgtv, full,
    gown, gpar, ring, usend, xs0, xs1, xs2, aown, apar, bmat, xfin, xback, sums,
    own_sem, mw_sem, gp_s, gp_r, ring_s, ring_r, a2a_s, a2a_r, yg_s, yg_r, half_s, half_r,
    xe_s, xe_r, ae_s, ae_r, bk_s, bk_r, ag_s, ag_r, ad_s, ad_r,
):
    nx, tp, mats, rows, cols = dims
    waves = mats // nx
    piece = rows // CHUNKS
    half = nx * rows
    width = tp * cols
    blk = min(256, half // 2)
    nblk = min(256, cols // 2)
    xs = (xs0, xs1)
    pong = xs2
    out_scale = 0.2 * math.sqrt(max(2 * half, width))

    d = lax.axis_index("dp")
    y = lax.axis_index("tp")
    x = d // 2
    c = d % 2
    turn = 1 - 2 * c
    nxt_x = (x + turn + nx) % nx
    partner = {"dp": 2 * x + (1 - c)}
    right = {"dp": 2 * nxt_x + c}

    my_cols = pl.ds(pl.multiple_of(y * cols, cols), cols)

    def at_x(dx):
        return {"dp": 2 * ((x + dx) % nx) + c}

    def at_y(dy):
        return {"tp": (y + dy) % tp}

    def remote(src, dst, send, recv, dev):
        return pltpu.make_async_remote_copy(
            src_ref=src, dst_ref=dst, send_sem=send, recv_sem=recv, device_id=dev, device_id_type=MESH
        )

    def all_of(like, sem):
        pltpu.make_async_copy(like, like, sem).wait()

    def wave(w):
        return pl.ds(w * nx, nx)

    def part(q):
        return pl.ds(q * piece, piece)

    def own_load(w, q):
        return pltpu.make_async_copy(
            grad.at[wave(w), :, c, part(q)], gown.at[wave(w), :, part(q)], own_sem.at[w, q]
        )

    def pair_copy(w, q):
        return remote(
            grad.at[wave(w), :, 1 - c, part(q)], gpar.at[wave(w), :, part(q)], gp_s.at[0], gp_r.at[w, q], partner
        )

    mom_load = pltpu.make_async_copy(mom, momv, mw_sem.at[0])
    wgt_load = pltpu.make_async_copy(wgt, wgtv, mw_sem.at[1])
    for w in range(waves):
        for q in range(CHUNKS):
            own_load(w, q).start()
    mom_load.start()
    wgt_load.start()

    barrier = pltpu.get_barrier_semaphore()
    peers = [partner] + [at_x(dx) for dx in range(1, nx)] + [at_y(dy) for dy in range(1, tp)]
    for peer in peers:
        pl.semaphore_signal(barrier, inc=1, device_id=peer, device_id_type=MESH)
    pl.semaphore_wait(barrier, len(peers))
    for w in range(waves):
        for q in range(CHUNKS):
            pair_copy(w, q).start()

    def ring_block(stage):
        return (x - turn * (1 + stage) + 4 * nx) % nx

    def ring_copy(w, q, stage):
        if stage == 0:
            src = gown.at[wave(w), ring_block(0), part(q)]
        else:
            src = ring.at[w, q, stage - 1]
        return remote(src, ring.at[w, q, stage], ring_s.at[0], ring_r.at[w, q, stage], right)

    def a2a_copy(w, q, dx):
        owner = (x + dx) % nx
        return remote(
            usend.at[w * nx + owner, part(q)],
            xs[w].at[0, x, part(q), my_cols],
            a2a_s.at[0], a2a_r.at[w, q], at_x(dx),
        )

    def ring_event(w, q, stage):
        block = ring_block(stage)
        if stage == 0:
            own_load(w, q).wait()
            pair_copy(w, q).wait_recv()
        else:
            ring_copy(w, q, stage - 1).wait_recv()
        for i in range(nx):
            m = w * nx + i
            local = gown[m, block, part(q)] + gpar[m, block, part(q)]
            if stage == 0:
                gown[m, block, part(q)] = local
            elif stage < nx - 1:
                ring[w, q, stage - 1, i] = ring[w, q, stage - 1, i] + local
            else:
                grad_mean = (ring[w, q, stage - 1, i] + local) * (1.0 / (2 * nx))
                mom_new = MOMENTUM * momv[m, part(q)] + grad_mean
                momv[m, part(q)] = mom_new
                usend[m, part(q)] = (grad_mean + MOMENTUM * mom_new).astype(BF16)
        if stage < nx - 1:
            ring_copy(w, q, stage).start()
        else:
            for dx in (2, 1, 3):
                a2a_copy(w, q, dx).start()
            xs[w][0, x, part(q), my_cols] = usend[w * nx + x, part(q)]

    def gather_copy(w, q, dy):
        region = xs[w].at[0, :, part(q), my_cols]
        return remote(region, region, yg_s.at[w], yg_r.at[w, q], at_y(dy))

    def half_copy(w, q):
        return remote(
            xs[w].at[0, :, part(q)], xs[w].at[1, :, part(q)], half_s.at[w], half_r.at[w, q], partner
        )

    def gather_event(w, q):
        all_of(usend.at[pl.ds(0, nx - 1), part(q)], a2a_r.at[w, q])
        for dy in (2, 1, 3):
            if dy < tp:
                gather_copy(w, q, dy).start()

    def add_squares(w, side, q):
        acc = sums[w]
        for i in range(nx):
            v = xs[w][side, i, part(q), :].astype(F32)
            v = v * v
            for n in range(width // 128):
                acc = acc + v[:, n * 128:(n + 1) * 128]
        sums[w] = acc

    def half_event(w, q):
        all_of(xs[w].at[0, :, part(q), pl.ds(0, width - cols)], yg_r.at[w, q])
        half_copy(w, q).start()
        add_squares(w, 0, q)

    def pair_event(w, q):
        half_copy(w, q).wait_recv()
        add_squares(w, 1, q)

    @scoped("normalise")
    def normalise(w):
        all_of(xs[w].at[0], half_s.at[w])
        all_of(xs[w].at[0, :, :, pl.ds(0, width - cols)], yg_s.at[w])
        total = jnp.sum(sums[w])
        inv = 1.0 / (jnp.sqrt(jnp.full((8, 128), total, F32)) + NORM_EPS)
        inv = inv[0:1, 0:1]

        def scale_rows(r, carry):
            sl = pl.ds(pl.multiple_of(r * 16, 16), 16)
            for side in range(2):
                for i in range(nx):
                    xs[w][side, i, sl, :] = (xs[w][side, i, sl, :].astype(F32) * inv).astype(BF16)
            return carry

        lax.fori_loop(0, rows // 16, scale_rows, 0)

    own = pl.ds(0, half)
    own_blocks = half // blk
    n_chunks = width // nblk
    batch = max(1, n_chunks // 2)

    def chunk_copy(dst, par, n):
        col = pl.ds(pl.multiple_of(n * nblk, nblk), nblk)
        return remote(dst.at[0, :, :, col], dst.at[1, :, :, col], xe_s.at[par], xe_r.at[par], partner)

    def newton_schulz(w, service):
        def a_copy(par):
            slot = (par + w) % 2
            return remote(aown.at[:, own], apar.at[slot], ae_s.at[slot], ae_r.at[slot], partner)

        def a_block(cur, side, j):
            per = blk // rows if blk >= rows else 1
            rhs = cur[side, j * per:(j + 1) * per].reshape(blk, width)
            lhs = cur[0].reshape(half, width)
            col = (side * own_blocks + j) * blk
            aown[:, col:col + blk] = dot_nt(lhs, rhs).astype(BF16)

        def b_own(j):
            rs = slice(j * blk, (j + 1) * blk)
            sq = dot_nt(aown[...], aown[rs, :])
            bmat[:, rs] = (COEF_B * aown[:, rs].astype(F32) + COEF_C * sq).astype(BF16)

        def b_other(par, j):
            rs = slice(j * blk, (j + 1) * blk)
            ps = slice(half + j * blk, half + (j + 1) * blk)
            sq = dot_nn(aown[:, :half], aown[:, ps]) + dot_nn(aown[:, half:], apar[(par + w) % 2, :, rs])
            bmat[:, ps] = (COEF_B * aown[:, ps].astype(F32) + COEF_C * sq).astype(BF16)

        def x_cols(cur, col):
            rhs = cur[:, :, :, col].reshape(2 * half, nblk)
            new = COEF_A * cur[0, :, :, col].reshape(half, nblk).astype(F32) + dot_nn(bmat[...], rhs)
            return new.astype(BF16)

        def iteration(it, par, cur, nxt, first, final):
            def drain_a():
                a_copy(1 - par).wait_send()

            def need_x():
                all_of(cur.at[0], xe_s.at[1 - par])
                all_of(cur.at[1], xe_r.at[1 - par])

            def guarded(fn):
                if first is False:
                    fn()
                else:
                    pl.when(jnp.logical_not(first))(fn)

            guarded(drain_a)
            with jax.named_scope("a_own"):
                for j in range(own_blocks):
                    a_block(cur, 0, j)
            a_copy(par).start()
            service(it, 0)
            with jax.named_scope("x_wait"):
                guarded(need_x)
            with jax.named_scope("a_other"):
                for j in range(own_blocks):
                    a_block(cur, 1, j)
            service(it, 1)
            with jax.named_scope("a_wait"):
                a_copy(par).wait_recv()
            with jax.named_scope("b_step"):
                for j in range(own_blocks):
                    b_own(j)
                for j in range(own_blocks):
                    b_other(par, j)
            service(it, 2)
            service(it, 3)
            if final:
                with jax.named_scope("x_last"):
                    for n in range(cols // nblk):
                        col = pl.ds(pl.multiple_of(y * cols + n * nblk, nblk), nblk)
                        xfin[w, :, :, n * nblk:(n + 1) * nblk] = x_cols(cur, col).reshape(nx, rows, nblk)
            else:
                def x_pair(k, carry):
                    cols_of = [pl.ds(pl.multiple_of((2 * k + e) * nblk, nblk), nblk) for e in range(2)]
                    for col in cols_of:
                        nxt[0, :, :, col] = x_cols(cur, col).reshape(nx, rows, nblk)
                    for e in range(2):
                        chunk_copy(nxt, par, 2 * k + e).start()
                    return carry

                for part_no in range(2):
                    with jax.named_scope("x_step"):
                        lax.fori_loop(part_no * batch // 2, (part_no + 1) * batch // 2, x_pair, 0)
                    service(it, 4 + part_no)

        def pair_of_steps(p, carry):
            iteration((p, 0), 0, xs[w], pong, p == 0, False)
            iteration((p, 1), 1, pong, xs[w], False, False)
            return carry

        lax.fori_loop(0, NS_STEPS // 2, pair_of_steps, 0)
        iteration(NS_STEPS - 1, 0, xs[w], None, False, True)
        a_copy(0).wait_send()

    def back_copy(w, dx):
        return remote(
            xfin.at[w, (x + dx) % nx],
            xback.at[w * nx + x], bk_s.at[0], bk_r.at[w, dx], at_x(dx),
        )

    def back_arrival(w, dx):
        m = w * nx + (x - dx + nx) % nx
        return remote(
            xfin.at[w, 0], xback.at[m], bk_s.at[0], bk_r.at[w, dx], at_x(dx)
        )

    def back_send(w):
        for dx in (2, 1, 3):
            back_copy(w, dx).start()
        xback[w * nx + x] = xfin[w, x]

    order = (0, 1, 3, 2)

    def gather_slot(w, hop, j):
        holder = (x - turn * hop + 4 * nx) % nx
        return holder, w * nx + (holder - order[j] + nx) % nx

    def ag_copy(w, hop, j):
        holder, m = gather_slot(w, hop, j)
        block = full.at[m, holder, c]
        return remote(block, block, ag_s.at[0], ag_r.at[m, hop], right)

    def ag_arrival(w, hop, j):
        holder, m = gather_slot(w, hop + 1, j)
        block = full.at[m, holder, c]
        return remote(block, block, ag_s.at[0], ag_r.at[m, hop], right)

    def pair_full(w, hop, j):
        holder, m = gather_slot(w, hop, j)
        block = full.at[m, holder, c]
        return remote(block, block, ad_s.at[0], ad_r.at[w], partner)

    def weight_event(w, j):
        dx = order[j]
        m = w * nx + (x - dx + nx) % nx
        if dx:
            back_arrival(w, dx).wait_recv()
        w_old = wgtv[m]
        w_new = w_old - rate[m] * (out_scale * xback[m].astype(F32) + decay[0] * w_old)
        wgtv[m] = w_new
        full[m, x, c] = w_new.astype(BF16)
        ag_copy(w, 0, j).start()
        pair_full(w, 0, j).start()

    def forward_event(w, hop, j):
        ag_arrival(w, hop - 1, j).wait_recv()
        if hop < nx - 1:
            ag_copy(w, hop, j).start()
        pair_full(w, hop, j).start()

    def finish_gather(w):
        all_of(full.at[wave(w), :, 1 - c], ad_r.at[w])

    handlers = {"ring": ring_event, "gather": gather_event, "half": half_event, "pair": pair_event}

    def perform(events):
        for kind, *rest in events:
            with jax.named_scope(kind + "#a=" + "_".join(str(a) for a in rest)):
                handlers[kind](*rest)

    def server(table):
        def service(it, slot):
            if isinstance(it, tuple):
                p, odd = it
                for k in range(NS_STEPS // 2):
                    work = table.get((2 * k + odd, slot), [])
                    if work:
                        pl.when(p == k)(functools.partial(perform, work))
            else:
                perform(table.get((it, slot), []))
        return service

    handlers["weight"] = weight_event
    handlers["forward"] = forward_event
    before, during, after = make_plan(waves, nx - 1)
    for w in range(waves):
        sums[w] = jnp.zeros((piece, 128), F32)
    mom_load.wait()
    perform(before)
    normalise(0)
    newton_schulz(0, server(during))
    back_send(0)
    wgt_load.wait()
    perform([e for e in after if e[0] in ("ring", "gather")])
    perform([("weight", 0, 0)])
    perform([e for e in after if e[0] in ("half", "pair")])
    normalise(1)
    second = {
        (0, 4): [("weight", 0, 1)], (0, 5): [("weight", 0, 2)], (1, 0): [("weight", 0, 3)],
        (1, 2): [("forward", 0, 1, 0)], (1, 3): [("forward", 0, 1, 1)],
        (1, 4): [("forward", 0, 1, 2)], (1, 5): [("forward", 0, 1, 3)],
        (2, 2): [("forward", 0, 2, 0)], (2, 3): [("forward", 0, 2, 1)],
        (2, 4): [("forward", 0, 2, 2)], (2, 5): [("forward", 0, 2, 3)],
        (3, 2): [("forward", 0, 3, 0)], (3, 3): [("forward", 0, 3, 1)],
        (3, 4): [("forward", 0, 3, 2)], (3, 5): [("forward", 0, 3, 3)],
    }
    newton_schulz(1, server(second))
    back_send(1)
    perform([("weight", 1, j) for j in range(nx)])
    perform([("forward", 1, hop, j) for hop in range(1, nx) for j in range(nx)])
    with jax.named_scope("finish"):
        for w in range(waves):
            finish_gather(w)

    all_of(gpar, gp_s.at[0])
    all_of(ring, ring_s.at[0])
    all_of(usend.at[pl.ds(0, waves * (nx - 1))], a2a_s.at[0])
    all_of(xback.at[pl.ds(0, waves * (nx - 1))], bk_s.at[0])
    all_of(full.at[:, pl.ds(0, nx - 1), 0], ag_s.at[0])
    all_of(full.at[:, :, 0], ad_s.at[0])


def store_kernel(a, b, c, a_out, b_out, c_out, sem):
    cut = a.shape[0] // 2
    pieces = [(c.at[m], c_out.at[m]) for m in range(c.shape[0])]
    for src, dst in ((a, a_out), (b, b_out)):
        pieces += [(src.at[pl.ds(k * cut, cut)], dst.at[pl.ds(k * cut, cut)]) for k in range(2)]
    copies = [pltpu.make_async_copy(src, dst, sem.at[i]) for i, (src, dst) in enumerate(pieces)]
    for copy in copies:
        copy.start()
    for copy in copies:
        copy.wait()


def solution(mesh):
    dp = mesh.shape["dp"]
    tp = mesh.shape["tp"]
    nx = dp // 2

    def local_step(grad_local, mom_local, weight_local, learn_rate, decay_rate):
        mats, rows, cols = mom_local.shape
        waves = mats // nx
        piece = rows // CHUNKS
        half = nx * rows
        width = tp * cols
        n_chunks = width // min(256, cols // 2)
        dma = pltpu.SemaphoreType.DMA
        vmem = pltpu.VMEM
        anyspec = pl.BlockSpec(memory_space=pl.ANY)
        smem = pl.BlockSpec(memory_space=pltpu.SMEM)
        vspec = pl.BlockSpec(memory_space=pltpu.VMEM)
        grad_view = grad_local.reshape(mats, nx, 2, rows, cols)
        call = pl.pallas_call(
            functools.partial(muon_kernel, (nx, tp, mats, rows, cols)),
            out_shape=(
                vmem((mats, rows, cols), F32),
                vmem((mats, rows, cols), F32),
                vmem((mats, nx, 2, rows, cols), BF16),
            ),
            in_specs=[anyspec, anyspec, anyspec, smem, smem],
            out_specs=(vspec, vspec, vspec),
            scratch_shapes=[
                vmem((mats, nx, rows, cols), F32),
                vmem((mats, nx, rows, cols), F32),
                vmem((waves, CHUNKS, nx - 1, nx, piece, cols), F32),
                vmem((mats, rows, cols), BF16),
                vmem((2, nx, rows, width), BF16),
                vmem((2, nx, rows, width), BF16),
                vmem((2, nx, rows, width), BF16),
                vmem((half, 2 * half), BF16),
                vmem((2, half, half), BF16),
                vmem((half, 2 * half), BF16),
                vmem((waves, nx, rows, cols), BF16),
                vmem((mats, rows, cols), BF16),
                vmem((waves, piece, 128), F32),
                dma((waves, CHUNKS)),
                dma((2,)),
                dma((1,)),
                dma((waves, CHUNKS)),
                dma((1,)),
                dma((waves, CHUNKS, nx - 1)),
                dma((1,)),
                dma((waves, CHUNKS)),
                dma((waves,)),
                dma((waves, CHUNKS)),
                dma((waves,)),
                dma((waves, CHUNKS)),
                dma((2,)),
                dma((2,)),
                dma((2,)),
                dma((2,)),
                dma((1,)),
                dma((waves, nx)),
                dma((1,)),
                dma((mats, nx - 1)),
                dma((1,)),
                dma((waves,)),
            ],
            compiler_params=pltpu.CompilerParams(
                collective_id=0, has_side_effects=True, vmem_limit_bytes=46 * 1024 * 1024
            ),
        )
        results = call(grad_view, mom_local, weight_local, learn_rate, decay_rate.reshape(1))
        results = [pltpu.with_memory_space_constraint(r, pltpu.VMEM) for r in results]
        mom_new, weight_new, full = pl.pallas_call(
            store_kernel,
            out_shape=tuple(jax.ShapeDtypeStruct(r.shape, r.dtype) for r in results),
            in_specs=[vspec] * 3,
            out_specs=(anyspec,) * 3,
            scratch_shapes=[dma((mats + 4,))],
            compiler_params=pltpu.CompilerParams(vmem_limit_bytes=1024 * 1024),
        )(*results)
        return mom_new, weight_new, full.reshape(mats, dp * rows, cols)

    return jax.shard_map(
        local_step,
        mesh=mesh,
        in_specs=(P(("rep", "dp"), None, None, "tp"), P("rep", "dp", "tp"), P("rep", "dp", "tp"), P("rep"), P()),
        out_specs=(P("rep", "dp", "tp"), P("rep", "dp", "tp"), P("rep", None, "tp")),
        check_vma=False,
    )
```

```python
import functools
import math

import jax
import jax.numpy as jnp
from jax import lax
from jax.experimental import pallas as pl
from jax.experimental.pallas import tpu as pltpu
from jax.sharding import PartitionSpec as P

MOMENTUM = 0.95
NS_STEPS = 5
COEF_A = 3.4445
COEF_B = -4.7750
COEF_C = 2.0315
NORM_EPS = 1e-7
MESH = pl.DeviceIdType.MESH
F32 = jnp.float32
BF16 = jnp.bfloat16
CHUNKS = 8
SLOTS = 6


def make_plan(waves, stages):
    wire, lat, gather_wire, small = 1.41, 2.0, 2.81, 0.7
    step = (1.4, 1.4, 1.5, 0.05, 1.68, 1.68)
    now, link, ylink = 2.0, 0.0, 0.0
    waiting = []
    fresh = [(w, q) for w in range(waves) for q in range(CHUNKS)]
    rank = {"ring": 0, "gather": 1, "half": 2, "pair": 3}

    def run(event):
        nonlocal now, link, ylink
        kind, w, q = event[:3]
        now += 0.06
        if kind == "ring" and event[3] < stages:
            link = max(link, now) + wire
            waiting.append((link + lat, ("ring", w, q, event[3] + 1)))
        elif kind == "ring":
            link = max(link, now) + small
            waiting.append((link + lat + 0.3, ("gather", w, q)))
        elif kind == "gather":
            ylink = max(ylink, now) + gather_wire
            waiting.append((ylink + lat + 1.5 * w, ("half", w, q)))
        elif kind == "half":
            waiting.append((now + 1.7, ("pair", w, q)))

    def take(limit, late=0.0):
        nonlocal now
        due = [item for item in waiting if item[0] <= limit - late * item[1][1]]
        if not due:
            return None
        best = min(due, key=lambda item: (item[1][1], rank[item[1][0]], item[0]))
        waiting.remove(best)
        now = max(now, best[0])
        return best[1]

    before, slots, after = [], {}, []
    todo = CHUNKS
    while todo:
        event = take(now, 1.5)
        usable, depth = False, 1.2
        if fresh and fresh[0][0]:
            started = len([e for e in before if e[1] and e[0] == "ring" and not e[3]])
            usable = ("ring", 0, CHUNKS - 1, stages - 1) in before and started < 1
            usable = usable or ("ring", 0, CHUNKS - 1, stages) in before
        elif fresh:
            usable = True
        if event is None and usable and link - now < depth:
            event = ("ring", *fresh.pop(0), 0)
        if event is None:
            times = [item[0] + 1.5 * item[1][1] for item in waiting]
            if usable:
                times.append(link - depth + 0.01)
            now = max(now + 0.01, min(times))
            continue
        run(event)
        before.append(event)
        todo -= event[0] == "pair" and event[1] == 0
    clock = now + 1.3
    for it in range(NS_STEPS):
        for slot in range(SLOTS if it < NS_STEPS - 1 else 4):
            clock += step[slot]
            now = clock
            found = []
            while True:
                event = take(now - 0.3)
                if event is None and fresh and link - now < 2.0:
                    event = ("ring", *fresh.pop(0), 0)
                if event is None:
                    break
                run(event)
                found.append(event)
            clock = now
            slots[it, slot] = found
    while fresh or waiting:
        if fresh:
            event = ("ring", *fresh.pop(0), 0)
        else:
            event = take(min(item[0] for item in waiting))
        run(event)
        after.append(event)
    return before, slots, after


def dot_nt(lhs, rhs):
    return lax.dot_general(lhs, rhs, (((1,), (1,)), ((), ())), preferred_element_type=F32)


def dot_nn(lhs, rhs):
    return jnp.dot(lhs, rhs, preferred_element_type=F32)


def muon_kernel(
    dims, grad, mom, wgt, rate, decay, momv, wgtv, full,
    gown, gpar, ring, usend, xs0, xs1, xs2, aown, apar, bmat, xfin, xback, sums,
    own_sem, mw_sem, gp_s, gp_r, ring_s, ring_r, a2a_s, a2a_r, yg_s, yg_r, half_s, half_r,
    xe_s, xe_r, ae_s, ae_r, bk_s, bk_r, ag_s, ag_r, ad_s, ad_r,
):
    nx, tp, mats, rows, cols = dims
    waves = mats // nx
    piece = rows // CHUNKS
    half = nx * rows
    width = tp * cols
    blk = min(256, half // 2)
    nblk = min(256, cols // 2)
    xs = (xs0, xs1)
    pong = xs2
    out_scale = 0.2 * math.sqrt(max(2 * half, width))

    d = lax.axis_index("dp")
    y = lax.axis_index("tp")
    x = d // 2
    c = d % 2
    turn = 1 - 2 * c
    nxt_x = (x + turn + nx) % nx
    partner = {"dp": 2 * x + (1 - c)}
    right = {"dp": 2 * nxt_x + c}

    my_cols = pl.ds(pl.multiple_of(y * cols, cols), cols)

    def at_x(dx):
        return {"dp": 2 * ((x + dx) % nx) + c}

    def at_y(dy):
        return {"tp": (y + dy) % tp}

    def remote(src, dst, send, recv, dev):
        return pltpu.make_async_remote_copy(
            src_ref=src, dst_ref=dst, send_sem=send, recv_sem=recv, device_id=dev, device_id_type=MESH
        )

    def all_of(like, sem):
        pltpu.make_async_copy(like, like, sem).wait()

    def wave(w):
        return pl.ds(w * nx, nx)

    def part(q):
        return pl.ds(q * piece, piece)

    def own_load(w, q):
        return pltpu.make_async_copy(
            grad.at[wave(w), :, c, part(q)], gown.at[wave(w), :, part(q)], own_sem.at[w, q]
        )

    def pair_copy(w, q):
        return remote(
            grad.at[wave(w), :, 1 - c, part(q)], gpar.at[wave(w), :, part(q)], gp_s.at[0], gp_r.at[w, q], partner
        )

    mom_load = pltpu.make_async_copy(mom, momv, mw_sem.at[0])
    wgt_load = pltpu.make_async_copy(wgt, wgtv, mw_sem.at[1])
    for w in range(waves):
        for q in range(CHUNKS):
            own_load(w, q).start()
    mom_load.start()
    wgt_load.start()

    barrier = pltpu.get_barrier_semaphore()
    peers = [partner] + [at_x(dx) for dx in range(1, nx)] + [at_y(dy) for dy in range(1, tp)]
    for peer in peers:
        pl.semaphore_signal(barrier, inc=1, device_id=peer, device_id_type=MESH)
    pl.semaphore_wait(barrier, len(peers))
    for w in range(waves):
        for q in range(CHUNKS):
            pair_copy(w, q).start()

    def ring_block(stage):
        return (x - turn * (1 + stage) + 4 * nx) % nx

    def ring_copy(w, q, stage):
        if stage == 0:
            src = gown.at[wave(w), ring_block(0), part(q)]
        else:
            src = ring.at[w, q, stage - 1]
        return remote(src, ring.at[w, q, stage], ring_s.at[0], ring_r.at[w, q, stage], right)

    def a2a_copy(w, q, dx):
        owner = (x + dx) % nx
        return remote(
            usend.at[w * nx + owner, part(q)],
            xs[w].at[0, x, part(q), my_cols],
            a2a_s.at[0], a2a_r.at[w, q], at_x(dx),
        )

    def ring_event(w, q, stage):
        block = ring_block(stage)
        if stage == 0:
            own_load(w, q).wait()
            pair_copy(w, q).wait_recv()
        else:
            ring_copy(w, q, stage - 1).wait_recv()
        for i in range(nx):
            m = w * nx + i
            local = gown[m, block, part(q)] + gpar[m, block, part(q)]
            if stage == 0:
                gown[m, block, part(q)] = local
            elif stage < nx - 1:
                ring[w, q, stage - 1, i] = ring[w, q, stage - 1, i] + local
            else:
                grad_mean = (ring[w, q, stage - 1, i] + local) * (1.0 / (2 * nx))
                mom_new = MOMENTUM * momv[m, part(q)] + grad_mean
                momv[m, part(q)] = mom_new
                usend[m, part(q)] = (grad_mean + MOMENTUM * mom_new).astype(BF16)
        if stage < nx - 1:
            ring_copy(w, q, stage).start()
        else:
            for dx in (2, 1, 3):
                a2a_copy(w, q, dx).start()
            xs[w][0, x, part(q), my_cols] = usend[w * nx + x, part(q)]

    def gather_copy(w, q, dy):
        region = xs[w].at[0, :, part(q), my_cols]
        return remote(region, region, yg_s.at[w], yg_r.at[w, q], at_y(dy))

    def half_copy(w, q):
        return remote(
            xs[w].at[0, :, part(q)], xs[w].at[1, :, part(q)], half_s.at[w], half_r.at[w, q], partner
        )

    def gather_event(w, q):
        all_of(usend.at[pl.ds(0, nx - 1), part(q)], a2a_r.at[w, q])
        for dy in (2, 1, 3):
            if dy < tp:
                gather_copy(w, q, dy).start()

    def add_squares(w, side, q):
        acc = sums[w]
        for i in range(nx):
            v = xs[w][side, i, part(q), :].astype(F32)
            v = v * v
            for n in range(width // 128):
                acc = acc + v[:, n * 128:(n + 1) * 128]
        sums[w] = acc

    def half_event(w, q):
        all_of(xs[w].at[0, :, part(q), pl.ds(0, width - cols)], yg_r.at[w, q])
        half_copy(w, q).start()
        add_squares(w, 0, q)

    def pair_event(w, q):
        half_copy(w, q).wait_recv()
        add_squares(w, 1, q)

    def normalise(w):
        all_of(xs[w].at[0], half_s.at[w])
        all_of(xs[w].at[0, :, :, pl.ds(0, width - cols)], yg_s.at[w])
        total = jnp.sum(sums[w])
        inv = 1.0 / (jnp.sqrt(jnp.full((8, 128), total, F32)) + NORM_EPS)
        inv = inv[0:1, 0:1]

        def scale_rows(r, carry):
            sl = pl.ds(pl.multiple_of(r * 16, 16), 16)
            for side in range(2):
                for i in range(nx):
                    xs[w][side, i, sl, :] = (xs[w][side, i, sl, :].astype(F32) * inv).astype(BF16)
            return carry

        lax.fori_loop(0, rows // 16, scale_rows, 0)

    own = pl.ds(0, half)
    own_blocks = half // blk
    n_chunks = width // nblk
    batch = max(1, n_chunks // 2)

    def chunk_copy(dst, par, n):
        col = pl.ds(pl.multiple_of(n * nblk, nblk), nblk)
        return remote(dst.at[0, :, :, col], dst.at[1, :, :, col], xe_s.at[par], xe_r.at[par], partner)

    def newton_schulz(w, service):
        def a_copy(par):
            slot = (par + w) % 2
            return remote(aown.at[:, own], apar.at[slot], ae_s.at[slot], ae_r.at[slot], partner)

        def a_block(cur, side, j):
            per = blk // rows if blk >= rows else 1
            rhs = cur[side, j * per:(j + 1) * per].reshape(blk, width)
            lhs = cur[0].reshape(half, width)
            col = (side * own_blocks + j) * blk
            aown[:, col:col + blk] = dot_nt(lhs, rhs).astype(BF16)

        def b_own(j):
            rs = slice(j * blk, (j + 1) * blk)
            sq = dot_nt(aown[...], aown[rs, :])
            bmat[:, rs] = (COEF_B * aown[:, rs].astype(F32) + COEF_C * sq).astype(BF16)

        def b_other(par, j):
            rs = slice(j * blk, (j + 1) * blk)
            ps = slice(half + j * blk, half + (j + 1) * blk)
            sq = dot_nn(aown[:, :half], aown[:, ps]) + dot_nn(aown[:, half:], apar[(par + w) % 2, :, rs])
            bmat[:, ps] = (COEF_B * aown[:, ps].astype(F32) + COEF_C * sq).astype(BF16)

        def x_cols(cur, col):
            rhs = cur[:, :, :, col].reshape(2 * half, nblk)
            new = COEF_A * cur[0, :, :, col].reshape(half, nblk).astype(F32) + dot_nn(bmat[...], rhs)
            return new.astype(BF16)

        def iteration(it, par, cur, nxt, first, final):
            def drain_a():
                a_copy(1 - par).wait_send()

            def need_x():
                all_of(cur.at[0], xe_s.at[1 - par])
                all_of(cur.at[1], xe_r.at[1 - par])

            def guarded(fn):
                if first is False:
                    fn()
                else:
                    pl.when(jnp.logical_not(first))(fn)

            guarded(drain_a)
            for j in range(own_blocks):
                a_block(cur, 0, j)
            a_copy(par).start()
            service(it, 0)
            guarded(need_x)
            for j in range(own_blocks):
                a_block(cur, 1, j)
            service(it, 1)
            a_copy(par).wait_recv()
            for j in range(own_blocks):
                b_own(j)
            for j in range(own_blocks):
                b_other(par, j)
            service(it, 2)
            service(it, 3)
            if final:
                for n in range(cols // nblk):
                    col = pl.ds(pl.multiple_of(y * cols + n * nblk, nblk), nblk)
                    xfin[w, :, :, n * nblk:(n + 1) * nblk] = x_cols(cur, col).reshape(nx, rows, nblk)
            else:
                def x_pair(k, carry):
                    cols_of = [pl.ds(pl.multiple_of((2 * k + e) * nblk, nblk), nblk) for e in range(2)]
                    for col in cols_of:
                        nxt[0, :, :, col] = x_cols(cur, col).reshape(nx, rows, nblk)
                    for e in range(2):
                        chunk_copy(nxt, par, 2 * k + e).start()
                    return carry

                for part_no in range(2):
                    lax.fori_loop(part_no * batch // 2, (part_no + 1) * batch // 2, x_pair, 0)
                    service(it, 4 + part_no)

        def pair_of_steps(p, carry):
            iteration((p, 0), 0, xs[w], pong, p == 0, False)
            iteration((p, 1), 1, pong, xs[w], False, False)
            return carry

        lax.fori_loop(0, NS_STEPS // 2, pair_of_steps, 0)
        iteration(NS_STEPS - 1, 0, xs[w], None, False, True)
        a_copy(0).wait_send()

    def back_copy(w, dx):
        return remote(
            xfin.at[w, (x + dx) % nx],
            xback.at[w * nx + x], bk_s.at[0], bk_r.at[w, dx], at_x(dx),
        )

    def back_arrival(w, dx):
        m = w * nx + (x - dx + nx) % nx
        return remote(
            xfin.at[w, 0], xback.at[m], bk_s.at[0], bk_r.at[w, dx], at_x(dx)
        )

    def back_send(w):
        for dx in (2, 1, 3):
            back_copy(w, dx).start()
        xback[w * nx + x] = xfin[w, x]

    order = (0, 1, 3, 2)

    def gather_slot(w, hop, j):
        holder = (x - turn * hop + 4 * nx) % nx
        return holder, w * nx + (holder - order[j] + nx) % nx

    def ag_copy(w, hop, j):
        holder, m = gather_slot(w, hop, j)
        block = full.at[m, holder, c]
        return remote(block, block, ag_s.at[0], ag_r.at[m, hop], right)

    def ag_arrival(w, hop, j):
        holder, m = gather_slot(w, hop + 1, j)
        block = full.at[m, holder, c]
        return remote(block, block, ag_s.at[0], ag_r.at[m, hop], right)

    def pair_full(w, hop, j):
        holder, m = gather_slot(w, hop, j)
        block = full.at[m, holder, c]
        return remote(block, block, ad_s.at[0], ad_r.at[w], partner)

    def weight_event(w, j):
        dx = order[j]
        m = w * nx + (x - dx + nx) % nx
        if dx:
            back_arrival(w, dx).wait_recv()
        w_old = wgtv[m]
        w_new = w_old - rate[m] * (out_scale * xback[m].astype(F32) + decay[0] * w_old)
        wgtv[m] = w_new
        full[m, x, c] = w_new.astype(BF16)
        ag_copy(w, 0, j).start()
        pair_full(w, 0, j).start()

    def forward_event(w, hop, j):
        ag_arrival(w, hop - 1, j).wait_recv()
        if hop < nx - 1:
            ag_copy(w, hop, j).start()
        pair_full(w, hop, j).start()

    def finish_gather(w):
        all_of(full.at[wave(w), :, 1 - c], ad_r.at[w])

    handlers = {"ring": ring_event, "gather": gather_event, "half": half_event, "pair": pair_event}

    def perform(events):
        for kind, *rest in events:
            handlers[kind](*rest)

    def server(table):
        def service(it, slot):
            if isinstance(it, tuple):
                p, odd = it
                for k in range(NS_STEPS // 2):
                    work = table.get((2 * k + odd, slot), [])
                    if work:
                        pl.when(p == k)(functools.partial(perform, work))
            else:
                perform(table.get((it, slot), []))
        return service

    handlers["weight"] = weight_event
    handlers["forward"] = forward_event
    before, during, after = make_plan(waves, nx - 1)
    for w in range(waves):
        sums[w] = jnp.zeros((piece, 128), F32)
    mom_load.wait()
    perform(before)
    normalise(0)
    newton_schulz(0, server(during))
    back_send(0)
    wgt_load.wait()
    perform([e for e in after if e[0] in ("ring", "gather")])
    perform([("weight", 0, 0)])
    perform([e for e in after if e[0] in ("half", "pair")])
    normalise(1)
    second = {
        (0, 4): [("weight", 0, 1)], (0, 5): [("weight", 0, 2)], (1, 0): [("weight", 0, 3)],
        (1, 2): [("forward", 0, 1, 0)], (1, 3): [("forward", 0, 1, 1)],
        (1, 4): [("forward", 0, 1, 2)], (1, 5): [("forward", 0, 1, 3)],
        (2, 2): [("forward", 0, 2, 0)], (2, 3): [("forward", 0, 2, 1)],
        (2, 4): [("forward", 0, 2, 2)], (2, 5): [("forward", 0, 2, 3)],
        (3, 2): [("forward", 0, 3, 0)], (3, 3): [("forward", 0, 3, 1)],
        (3, 4): [("forward", 0, 3, 2)], (3, 5): [("forward", 0, 3, 3)],
    }
    newton_schulz(1, server(second))
    back_send(1)
    perform([("weight", 1, j) for j in range(nx)])
    perform([("forward", 1, hop, j) for hop in range(1, nx) for j in range(nx)])
    for w in range(waves):
        finish_gather(w)

    all_of(gpar, gp_s.at[0])
    all_of(ring, ring_s.at[0])
    all_of(usend.at[pl.ds(0, waves * (nx - 1))], a2a_s.at[0])
    all_of(xback.at[pl.ds(0, waves * (nx - 1))], bk_s.at[0])
    all_of(full.at[:, pl.ds(0, nx - 1), 0], ag_s.at[0])
    all_of(full.at[:, :, 0], ad_s.at[0])


def store_kernel(a, b, c, a_out, b_out, c_out, sem):
    cut = a.shape[0] // 2
    pieces = [(c.at[m], c_out.at[m]) for m in range(c.shape[0])]
    for src, dst in ((a, a_out), (b, b_out)):
        pieces += [(src.at[pl.ds(k * cut, cut)], dst.at[pl.ds(k * cut, cut)]) for k in range(2)]
    copies = [pltpu.make_async_copy(src, dst, sem.at[i]) for i, (src, dst) in enumerate(pieces)]
    for copy in copies:
        copy.start()
    for copy in copies:
        copy.wait()


def solution(mesh):
    dp = mesh.shape["dp"]
    tp = mesh.shape["tp"]
    nx = dp // 2

    def local_step(grad_local, mom_local, weight_local, learn_rate, decay_rate):
        mats, rows, cols = mom_local.shape
        waves = mats // nx
        piece = rows // CHUNKS
        half = nx * rows
        width = tp * cols
        n_chunks = width // min(256, cols // 2)
        dma = pltpu.SemaphoreType.DMA
        vmem = pltpu.VMEM
        anyspec = pl.BlockSpec(memory_space=pl.ANY)
        smem = pl.BlockSpec(memory_space=pltpu.SMEM)
        vspec = pl.BlockSpec(memory_space=pltpu.VMEM)
        grad_view = grad_local.reshape(mats, nx, 2, rows, cols)
        call = pl.pallas_call(
            functools.partial(muon_kernel, (nx, tp, mats, rows, cols)),
            out_shape=(
                vmem((mats, rows, cols), F32),
                vmem((mats, rows, cols), F32),
                vmem((mats, nx, 2, rows, cols), BF16),
            ),
            in_specs=[anyspec, anyspec, anyspec, smem, smem],
            out_specs=(vspec, vspec, vspec),
            scratch_shapes=[
                vmem((mats, nx, rows, cols), F32),
                vmem((mats, nx, rows, cols), F32),
                vmem((waves, CHUNKS, nx - 1, nx, piece, cols), F32),
                vmem((mats, rows, cols), BF16),
                vmem((2, nx, rows, width), BF16),
                vmem((2, nx, rows, width), BF16),
                vmem((2, nx, rows, width), BF16),
                vmem((half, 2 * half), BF16),
                vmem((2, half, half), BF16),
                vmem((half, 2 * half), BF16),
                vmem((waves, nx, rows, cols), BF16),
                vmem((mats, rows, cols), BF16),
                vmem((waves, piece, 128), F32),
                dma((waves, CHUNKS)),
                dma((2,)),
                dma((1,)),
                dma((waves, CHUNKS)),
                dma((1,)),
                dma((waves, CHUNKS, nx - 1)),
                dma((1,)),
                dma((waves, CHUNKS)),
                dma((waves,)),
                dma((waves, CHUNKS)),
                dma((waves,)),
                dma((waves, CHUNKS)),
                dma((2,)),
                dma((2,)),
                dma((2,)),
                dma((2,)),
                dma((1,)),
                dma((waves, nx)),
                dma((1,)),
                dma((mats, nx - 1)),
                dma((1,)),
                dma((waves,)),
            ],
            compiler_params=pltpu.CompilerParams(
                collective_id=0, has_side_effects=True, vmem_limit_bytes=46 * 1024 * 1024
            ),
        )
        results = call(grad_view, mom_local, weight_local, learn_rate, decay_rate.reshape(1))
        results = [pltpu.with_memory_space_constraint(r, pltpu.VMEM) for r in results]
        mom_new, weight_new, full = pl.pallas_call(
            store_kernel,
            out_shape=tuple(jax.ShapeDtypeStruct(r.shape, r.dtype) for r in results),
            in_specs=[vspec] * 3,
            out_specs=(anyspec,) * 3,
            scratch_shapes=[dma((mats + 4,))],
            compiler_params=pltpu.CompilerParams(vmem_limit_bytes=1024 * 1024),
        )(*results)
        return mom_new, weight_new, full.reshape(mats, dp * rows, cols)

    return jax.shard_map(
        local_step,
        mesh=mesh,
        in_specs=(P(("rep", "dp"), None, None, "tp"), P("rep", "dp", "tp"), P("rep", "dp", "tp"), P("rep"), P()),
        out_specs=(P("rep", "dp", "tp"), P("rep", "dp", "tp"), P("rep", None, "tp")),
        check_vma=False,
    )
```

```python
import functools
import math

import jax
import jax.numpy as jnp
from jax import lax
from jax.experimental import pallas as pl
from jax.experimental.pallas import tpu as pltpu
from jax.sharding import PartitionSpec as P

MOMENTUM = 0.95
NS_STEPS = 5
COEF_A = 3.4445
COEF_B = -4.7750
COEF_C = 2.0315
NORM_EPS = 1e-7
MESH = pl.DeviceIdType.MESH
F32 = jnp.float32
BF16 = jnp.bfloat16
CHUNKS = 8
SLOTS = 6


def make_plan(waves, stages):
    wire, lat, gather_wire, small = 1.41, 2.4, 2.81, 0.7
    step = (1.4, 1.4, 1.5, 0.05, 1.68, 1.68)
    now, link, ylink = 2.0, 0.0, 0.0
    waiting = []
    fresh = [(w, q) for w in range(waves) for q in range(CHUNKS)]
    rank = {"ring": 0, "gather": 1, "half": 2, "pair": 3}

    def run(event):
        nonlocal now, link, ylink
        kind, w, q = event[:3]
        now += 0.06
        if kind == "ring" and event[3] < stages:
            link = max(link, now) + wire
            waiting.append((link + lat, ("ring", w, q, event[3] + 1)))
        elif kind == "ring":
            link = max(link, now) + small
            waiting.append((link + lat + 0.3, ("gather", w, q)))
        elif kind == "gather":
            ylink = max(ylink, now) + gather_wire
            waiting.append((ylink + lat + 1.5 * w, ("half", w, q)))
        elif kind == "half":
            waiting.append((now + 1.7, ("pair", w, q)))

    def take(limit, late=0.0):
        nonlocal now
        due = [item for item in waiting if item[0] <= limit - late * item[1][1]]
        if not due:
            return None
        best = min(due, key=lambda item: (item[1][1], rank[item[1][0]], item[0]))
        waiting.remove(best)
        now = max(now, best[0])
        return best[1]

    before, slots, after = [], {}, []
    todo = CHUNKS
    while todo:
        event = take(now, 1.5)
        usable, depth = False, 2.0
        if fresh and fresh[0][0]:
            started = len([e for e in before if e[1] and e[0] == "ring" and not e[3]])
            usable = ("ring", 0, CHUNKS - 1, stages) in before and started < 4
        elif fresh:
            usable = True
        if event is None and usable and link - now < depth:
            event = ("ring", *fresh.pop(0), 0)
        if event is None:
            times = [item[0] + 1.5 * item[1][1] for item in waiting]
            if usable:
                times.append(link - depth + 0.01)
            now = max(now + 0.01, min(times))
            continue
        run(event)
        before.append(event)
        todo -= event[0] == "pair" and event[1] == 0
    clock, lat = now + 1.3, 2.1
    for it in range(NS_STEPS):
        for slot in range(SLOTS if it < NS_STEPS - 1 else 4):
            clock += step[slot]
            now = clock
            found = []
            while True:
                event = take(now - 0.1)
                if event is None and fresh and link - now < 2.5:
                    event = ("ring", *fresh.pop(0), 0)
                if event is None:
                    break
                run(event)
                found.append(event)
            clock = now
            slots[it, slot] = found
    while fresh or waiting:
        if fresh:
            event = ("ring", *fresh.pop(0), 0)
        else:
            event = take(min(item[0] for item in waiting))
        run(event)
        after.append(event)
    return before, slots, after


def dot_nt(lhs, rhs):
    return lax.dot_general(lhs, rhs, (((1,), (1,)), ((), ())), preferred_element_type=F32)


def dot_nn(lhs, rhs):
    return jnp.dot(lhs, rhs, preferred_element_type=F32)


def muon_kernel(
    dims, grad, mom, wgt, rate, decay, momv, wgtv, full,
    gown, gpar, ring, usend, xs0, xs1, xs2, aown, apar, bmat, xfin, xback, sums,
    own_sem, mw_sem, gp_s, gp_r, ring_s, ring_r, a2a_s, a2a_r, yg_s, yg_r, half_s, half_r,
    xe_s, xe_r, ae_s, ae_r, bk_s, bk_r, ag_s, ag_r, ad_s, ad_r,
):
    nx, tp, mats, rows, cols = dims
    waves = mats // nx
    piece = rows // CHUNKS
    half = nx * rows
    width = tp * cols
    blk = min(256, half // 2)
    nblk = min(256, cols // 2)
    xs = (xs0, xs1)
    pong = xs2
    out_scale = 0.2 * math.sqrt(max(2 * half, width))

    d = lax.axis_index("dp")
    y = lax.axis_index("tp")
    x = d // 2
    c = d % 2
    turn = 1 - 2 * c
    nxt_x = (x + turn + nx) % nx
    partner = {"dp": 2 * x + (1 - c)}
    right = {"dp": 2 * nxt_x + c}

    my_cols = pl.ds(pl.multiple_of(y * cols, cols), cols)

    def at_x(dx):
        return {"dp": 2 * ((x + dx) % nx) + c}

    def at_y(dy):
        return {"tp": (y + dy) % tp}

    def remote(src, dst, send, recv, dev):
        return pltpu.make_async_remote_copy(
            src_ref=src, dst_ref=dst, send_sem=send, recv_sem=recv, device_id=dev, device_id_type=MESH
        )

    def all_of(like, sem):
        pltpu.make_async_copy(like, like, sem).wait()

    def wave(w):
        return pl.ds(w * nx, nx)

    def part(q):
        return pl.ds(q * piece, piece)

    def own_load(w, q):
        return pltpu.make_async_copy(
            grad.at[wave(w), :, c, part(q)], gown.at[wave(w), :, part(q)], own_sem.at[w, q]
        )

    def pair_copy(w, q):
        return remote(
            grad.at[wave(w), :, 1 - c, part(q)], gpar.at[wave(w), :, part(q)], gp_s.at[0], gp_r.at[w, q], partner
        )

    mom_load = pltpu.make_async_copy(mom, momv, mw_sem.at[0])
    wgt_load = pltpu.make_async_copy(wgt, wgtv, mw_sem.at[1])
    for w in range(waves):
        for q in range(CHUNKS):
            own_load(w, q).start()
    mom_load.start()
    wgt_load.start()

    barrier = pltpu.get_barrier_semaphore()
    peers = [partner] + [at_x(dx) for dx in range(1, nx)] + [at_y(dy) for dy in range(1, tp)]
    for peer in peers:
        pl.semaphore_signal(barrier, inc=1, device_id=peer, device_id_type=MESH)
    pl.semaphore_wait(barrier, len(peers))
    for w in range(waves):
        for q in range(CHUNKS):
            pair_copy(w, q).start()

    def ring_block(stage):
        return (x - turn * (1 + stage) + 4 * nx) % nx

    def ring_copy(w, q, stage):
        if stage == 0:
            src = gown.at[wave(w), ring_block(0), part(q)]
        else:
            src = ring.at[w, q, stage - 1]
        return remote(src, ring.at[w, q, stage], ring_s.at[0], ring_r.at[w, q, stage], right)

    def a2a_copy(w, q, dx):
        owner = (x + dx) % nx
        return remote(
            usend.at[w * nx + owner, part(q)],
            xs[w].at[0, x, part(q), my_cols],
            a2a_s.at[0], a2a_r.at[w, q], at_x(dx),
        )

    def ring_event(w, q, stage):
        block = ring_block(stage)
        if stage == 0:
            own_load(w, q).wait()
            pair_copy(w, q).wait_recv()
        else:
            ring_copy(w, q, stage - 1).wait_recv()
        for i in range(nx):
            m = w * nx + i
            local = gown[m, block, part(q)] + gpar[m, block, part(q)]
            if stage == 0:
                gown[m, block, part(q)] = local
            elif stage < nx - 1:
                ring[w, q, stage - 1, i] = ring[w, q, stage - 1, i] + local
            else:
                grad_mean = (ring[w, q, stage - 1, i] + local) * (1.0 / (2 * nx))
                mom_new = MOMENTUM * momv[m, part(q)] + grad_mean
                momv[m, part(q)] = mom_new
                usend[m, part(q)] = (grad_mean + MOMENTUM * mom_new).astype(BF16)
        if stage < nx - 1:
            ring_copy(w, q, stage).start()
        else:
            for dx in (2, 1, 3):
                a2a_copy(w, q, dx).start()
            xs[w][0, x, part(q), my_cols] = usend[w * nx + x, part(q)]

    def gather_copy(w, q, dy):
        region = xs[w].at[0, :, part(q), my_cols]
        return remote(region, region, yg_s.at[w], yg_r.at[w, q], at_y(dy))

    def half_copy(w, q):
        return remote(
            xs[w].at[0, :, part(q)], xs[w].at[1, :, part(q)], half_s.at[w], half_r.at[w, q], partner
        )

    def gather_event(w, q):
        all_of(usend.at[pl.ds(0, nx - 1), part(q)], a2a_r.at[w, q])
        for dy in (2, 1, 3):
            if dy < tp:
                gather_copy(w, q, dy).start()

    def add_squares(w, side, q):
        acc = sums[w]
        for i in range(nx):
            v = xs[w][side, i, part(q), :].astype(F32)
            v = v * v
            for n in range(width // 128):
                acc = acc + v[:, n * 128:(n + 1) * 128]
        sums[w] = acc

    def half_event(w, q):
        all_of(xs[w].at[0, :, part(q), pl.ds(0, width - cols)], yg_r.at[w, q])
        half_copy(w, q).start()
        add_squares(w, 0, q)

    def pair_event(w, q):
        half_copy(w, q).wait_recv()
        add_squares(w, 1, q)

    def normalise(w):
        all_of(xs[w].at[0], half_s.at[w])
        all_of(xs[w].at[0, :, :, pl.ds(0, width - cols)], yg_s.at[w])
        total = jnp.sum(sums[w])
        inv = 1.0 / (jnp.sqrt(jnp.full((8, 128), total, F32)) + NORM_EPS)
        inv = inv[0:1, 0:1]

        def scale_rows(r, carry):
            sl = pl.ds(pl.multiple_of(r * 16, 16), 16)
            for side in range(2):
                for i in range(nx):
                    xs[w][side, i, sl, :] = (xs[w][side, i, sl, :].astype(F32) * inv).astype(BF16)
            return carry

        lax.fori_loop(0, rows // 16, scale_rows, 0)

    own = pl.ds(0, half)
    own_blocks = half // blk
    n_chunks = width // nblk
    batch = max(1, n_chunks // 2)

    def chunk_copy(dst, par, n):
        col = pl.ds(pl.multiple_of(n * nblk, nblk), nblk)
        return remote(dst.at[0, :, :, col], dst.at[1, :, :, col], xe_s.at[par], xe_r.at[par], partner)

    def newton_schulz(w, service):
        def a_copy(par):
            slot = (par + w) % 2
            return remote(aown.at[:, own], apar.at[slot], ae_s.at[slot], ae_r.at[slot], partner)

        def a_block(cur, side, j):
            per = blk // rows if blk >= rows else 1
            rhs = cur[side, j * per:(j + 1) * per].reshape(blk, width)
            lhs = cur[0].reshape(half, width)
            col = (side * own_blocks + j) * blk
            aown[:, col:col + blk] = dot_nt(lhs, rhs).astype(BF16)

        def b_own(j):
            rs = slice(j * blk, (j + 1) * blk)
            sq = dot_nt(aown[...], aown[rs, :])
            bmat[:, rs] = (COEF_B * aown[:, rs].astype(F32) + COEF_C * sq).astype(BF16)

        def b_other(par, j):
            rs = slice(j * blk, (j + 1) * blk)
            ps = slice(half + j * blk, half + (j + 1) * blk)
            sq = dot_nn(aown[:, :half], aown[:, ps]) + dot_nn(aown[:, half:], apar[(par + w) % 2, :, rs])
            bmat[:, ps] = (COEF_B * aown[:, ps].astype(F32) + COEF_C * sq).astype(BF16)

        def x_cols(cur, col):
            rhs = cur[:, :, :, col].reshape(2 * half, nblk)
            new = COEF_A * cur[0, :, :, col].reshape(half, nblk).astype(F32) + dot_nn(bmat[...], rhs)
            return new.astype(BF16)

        def iteration(it, par, cur, nxt, first, final):
            def drain_a():
                a_copy(1 - par).wait_send()

            def need_x():
                all_of(cur.at[0], xe_s.at[1 - par])
                all_of(cur.at[1], xe_r.at[1 - par])

            def guarded(fn):
                if first is False:
                    fn()
                else:
                    pl.when(jnp.logical_not(first))(fn)

            guarded(drain_a)
            for j in range(own_blocks):
                a_block(cur, 0, j)
            a_copy(par).start()
            service(it, 0)
            guarded(need_x)
            for j in range(own_blocks):
                a_block(cur, 1, j)
            service(it, 1)
            a_copy(par).wait_recv()
            for j in range(own_blocks):
                b_own(j)
            for j in range(own_blocks):
                b_other(par, j)
            service(it, 2)
            service(it, 3)
            if final:
                for n in range(cols // nblk):
                    col = pl.ds(pl.multiple_of(y * cols + n * nblk, nblk), nblk)
                    xfin[w, :, :, n * nblk:(n + 1) * nblk] = x_cols(cur, col).reshape(nx, rows, nblk)
            else:
                def x_pair(k, carry):
                    cols_of = [pl.ds(pl.multiple_of((2 * k + e) * nblk, nblk), nblk) for e in range(2)]
                    for col in cols_of:
                        nxt[0, :, :, col] = x_cols(cur, col).reshape(nx, rows, nblk)
                    for e in range(2):
                        chunk_copy(nxt, par, 2 * k + e).start()
                    return carry

                for part_no in range(2):
                    lax.fori_loop(part_no * batch // 2, (part_no + 1) * batch // 2, x_pair, 0)
                    service(it, 4 + part_no)

        def pair_of_steps(p, carry):
            iteration((p, 0), 0, xs[w], pong, p == 0, False)
            iteration((p, 1), 1, pong, xs[w], False, False)
            return carry

        lax.fori_loop(0, NS_STEPS // 2, pair_of_steps, 0)
        iteration(NS_STEPS - 1, 0, xs[w], None, False, True)
        a_copy(0).wait_send()

    def back_copy(w, dx):
        return remote(
            xfin.at[w, (x + dx) % nx],
            xback.at[w * nx + x], bk_s.at[0], bk_r.at[w, dx], at_x(dx),
        )

    def back_arrival(w, dx):
        m = w * nx + (x - dx + nx) % nx
        return remote(
            xfin.at[w, 0], xback.at[m], bk_s.at[0], bk_r.at[w, dx], at_x(dx)
        )

    def back_send(w):
        for dx in (1, 3, 2):
            back_copy(w, dx).start()
        xback[w * nx + x] = xfin[w, x]

    order = (0, 1, 3, 2)

    def gather_slot(w, hop, j):
        holder = (x - turn * hop + 4 * nx) % nx
        return holder, w * nx + (holder - order[j] + nx) % nx

    def ag_copy(w, hop, j):
        holder, m = gather_slot(w, hop, j)
        block = full.at[m, holder, c]
        return remote(block, block, ag_s.at[0], ag_r.at[m, hop], right)

    def ag_arrival(w, hop, j):
        holder, m = gather_slot(w, hop + 1, j)
        block = full.at[m, holder, c]
        return remote(block, block, ag_s.at[0], ag_r.at[m, hop], right)

    def pair_full(w, hop, j):
        holder, m = gather_slot(w, hop, j)
        block = full.at[m, holder, c]
        return remote(block, block, ad_s.at[0], ad_r.at[w], partner)

    def weight_event(w, j):
        dx = order[j]
        m = w * nx + (x - dx + nx) % nx
        if dx:
            back_arrival(w, dx).wait_recv()
        w_old = wgtv[m]
        w_new = w_old - rate[m] * (out_scale * xback[m].astype(F32) + decay[0] * w_old)
        wgtv[m] = w_new
        full[m, x, c] = w_new.astype(BF16)
        ag_copy(w, 0, j).start()
        pair_full(w, 0, j).start()

    def forward_event(w, hop, j):
        ag_arrival(w, hop - 1, j).wait_recv()
        if hop < nx - 1:
            ag_copy(w, hop, j).start()
        pair_full(w, hop, j).start()

    def finish_gather(w):
        all_of(full.at[wave(w), :, 1 - c], ad_r.at[w])

    handlers = {"ring": ring_event, "gather": gather_event, "half": half_event, "pair": pair_event}

    def perform(events):
        for kind, *rest in events:
            handlers[kind](*rest)

    def server(table):
        def service(it, slot):
            if isinstance(it, tuple):
                p, odd = it
                for k in range(NS_STEPS // 2):
                    work = table.get((2 * k + odd, slot), [])
                    if work:
                        pl.when(p == k)(functools.partial(perform, work))
            else:
                perform(table.get((it, slot), []))
        return service

    handlers["weight"] = weight_event
    handlers["forward"] = forward_event
    before, during, after = make_plan(waves, nx - 1)
    for w in range(waves):
        sums[w] = jnp.zeros((piece, 128), F32)
    mom_load.wait()
    perform(before)
    normalise(0)
    newton_schulz(0, server(during))
    back_send(0)
    wgt_load.wait()
    perform([e for e in after if e[0] in ("ring", "gather")])
    perform([("weight", 0, 0)])
    perform([e for e in after if e[0] in ("half", "pair")])
    normalise(1)
    second = {
        (0, 4): [("weight", 0, 1)], (0, 5): [("weight", 0, 2)], (1, 0): [("weight", 0, 3)],
        (1, 2): [("forward", 0, 1, 0)], (1, 3): [("forward", 0, 1, 1)],
        (1, 4): [("forward", 0, 1, 2)], (1, 5): [("forward", 0, 1, 3)],
        (2, 2): [("forward", 0, 2, 0)], (2, 3): [("forward", 0, 2, 1)],
        (2, 4): [("forward", 0, 2, 2)], (2, 5): [("forward", 0, 2, 3)],
        (3, 2): [("forward", 0, 3, 0)], (3, 3): [("forward", 0, 3, 1)],
        (3, 4): [("forward", 0, 3, 2)], (3, 5): [("forward", 0, 3, 3)],
    }
    newton_schulz(1, server(second))
    back_send(1)
    perform([("weight", 1, j) for j in range(nx)])
    perform([("forward", 1, hop, j) for hop in range(1, nx) for j in range(nx)])
    for w in range(waves):
        finish_gather(w)

    all_of(gpar, gp_s.at[0])
    all_of(ring, ring_s.at[0])
    all_of(usend.at[pl.ds(0, waves * (nx - 1))], a2a_s.at[0])
    all_of(xback.at[pl.ds(0, waves * (nx - 1))], bk_s.at[0])
    all_of(full.at[:, pl.ds(0, nx - 1), 0], ag_s.at[0])
    all_of(full.at[:, :, 0], ad_s.at[0])


def store_kernel(a, b, c, a_out, b_out, c_out, sem):
    cut = a.shape[0] // 2
    pieces = [(c.at[m], c_out.at[m]) for m in range(c.shape[0])]
    for src, dst in ((a, a_out), (b, b_out)):
        pieces += [(src.at[pl.ds(k * cut, cut)], dst.at[pl.ds(k * cut, cut)]) for k in range(2)]
    copies = [pltpu.make_async_copy(src, dst, sem.at[i]) for i, (src, dst) in enumerate(pieces)]
    for copy in copies:
        copy.start()
    for copy in copies:
        copy.wait()


def solution(mesh):
    dp = mesh.shape["dp"]
    tp = mesh.shape["tp"]
    nx = dp // 2

    def local_step(grad_local, mom_local, weight_local, learn_rate, decay_rate):
        mats, rows, cols = mom_local.shape
        waves = mats // nx
        piece = rows // CHUNKS
        half = nx * rows
        width = tp * cols
        n_chunks = width // min(256, cols // 2)
        dma = pltpu.SemaphoreType.DMA
        vmem = pltpu.VMEM
        anyspec = pl.BlockSpec(memory_space=pl.ANY)
        smem = pl.BlockSpec(memory_space=pltpu.SMEM)
        vspec = pl.BlockSpec(memory_space=pltpu.VMEM)
        grad_view = grad_local.reshape(mats, nx, 2, rows, cols)
        call = pl.pallas_call(
            functools.partial(muon_kernel, (nx, tp, mats, rows, cols)),
            out_shape=(
                vmem((mats, rows, cols), F32),
                vmem((mats, rows, cols), F32),
                vmem((mats, nx, 2, rows, cols), BF16),
            ),
            in_specs=[anyspec, anyspec, anyspec, smem, smem],
            out_specs=(vspec, vspec, vspec),
            scratch_shapes=[
                vmem((mats, nx, rows, cols), F32),
                vmem((mats, nx, rows, cols), F32),
                vmem((waves, CHUNKS, nx - 1, nx, piece, cols), F32),
                vmem((mats, rows, cols), BF16),
                vmem((2, nx, rows, width), BF16),
                vmem((2, nx, rows, width), BF16),
                vmem((2, nx, rows, width), BF16),
                vmem((half, 2 * half), BF16),
                vmem((2, half, half), BF16),
                vmem((half, 2 * half), BF16),
                vmem((waves, nx, rows, cols), BF16),
                vmem((mats, rows, cols), BF16),
                vmem((waves, piece, 128), F32),
                dma((waves, CHUNKS)),
                dma((2,)),
                dma((1,)),
                dma((waves, CHUNKS)),
                dma((1,)),
                dma((waves, CHUNKS, nx - 1)),
                dma((1,)),
                dma((waves, CHUNKS)),
                dma((waves,)),
                dma((waves, CHUNKS)),
                dma((waves,)),
                dma((waves, CHUNKS)),
                dma((2,)),
                dma((2,)),
                dma((2,)),
                dma((2,)),
                dma((1,)),
                dma((waves, nx)),
                dma((1,)),
                dma((mats, nx - 1)),
                dma((1,)),
                dma((waves,)),
            ],
            compiler_params=pltpu.CompilerParams(
                collective_id=0, has_side_effects=True, vmem_limit_bytes=46 * 1024 * 1024
            ),
        )
        results = call(grad_view, mom_local, weight_local, learn_rate, decay_rate.reshape(1))
        results = [pltpu.with_memory_space_constraint(r, pltpu.VMEM) for r in results]
        mom_new, weight_new, full = pl.pallas_call(
            store_kernel,
            out_shape=tuple(jax.ShapeDtypeStruct(r.shape, r.dtype) for r in results),
            in_specs=[vspec] * 3,
            out_specs=(anyspec,) * 3,
            scratch_shapes=[dma((mats + 4,))],
            compiler_params=pltpu.CompilerParams(vmem_limit_bytes=1024 * 1024),
        )(*results)
        return mom_new, weight_new, full.reshape(mats, dp * rows, cols)

    return jax.shard_map(
        local_step,
        mesh=mesh,
        in_specs=(P(("rep", "dp"), None, None, "tp"), P("rep", "dp", "tp"), P("rep", "dp", "tp"), P("rep"), P()),
        out_specs=(P("rep", "dp", "tp"), P("rep", "dp", "tp"), P("rep", None, "tp")),
        check_vma=False,
    )
```

```python
import functools
import math

import jax
import jax.numpy as jnp
from jax import lax
from jax.experimental import pallas as pl
from jax.experimental.pallas import tpu as pltpu
from jax.sharding import PartitionSpec as P

MOMENTUM = 0.95
NS_STEPS = 5
COEF_A = 3.4445
COEF_B = -4.7750
COEF_C = 2.0315
NORM_EPS = 1e-7
MESH = pl.DeviceIdType.MESH
F32 = jnp.float32
BF16 = jnp.bfloat16
CHUNKS = 8
SLOTS = 6


def make_plan(waves, stages):
    wire, lat, gather_wire, small = 1.41, 2.0, 2.81, 0.7
    step = (1.4, 1.4, 1.5, 0.05, 1.68, 1.68)
    now, link, ylink = 2.0, 0.0, 0.0
    waiting = []
    fresh = [(w, q) for w in range(waves) for q in range(CHUNKS)]
    rank = {"ring": 0, "gather": 1, "half": 2, "pair": 3}

    def run(event):
        nonlocal now, link, ylink
        kind, w, q = event[:3]
        now += 0.06
        if kind == "ring" and event[3] < stages:
            link = max(link, now) + wire
            waiting.append((link + lat, ("ring", w, q, event[3] + 1)))
        elif kind == "ring":
            link = max(link, now) + small
            waiting.append((link + lat + 0.3, ("gather", w, q)))
        elif kind == "gather":
            ylink = max(ylink, now) + gather_wire
            waiting.append((ylink + lat + 1.5 * w, ("half", w, q)))
        elif kind == "half":
            waiting.append((now + 1.7, ("pair", w, q)))

    def take(limit, late=0.0):
        nonlocal now
        due = [item for item in waiting if item[0] <= limit - late * item[1][1]]
        if not due:
            return None
        best = min(due, key=lambda item: (item[1][1], rank[item[1][0]], item[0]))
        waiting.remove(best)
        now = max(now, best[0])
        return best[1]

    before, slots, after = [], {}, []
    todo = CHUNKS
    while todo:
        event = take(now, 1.5)
        usable, depth = False, 1.2
        if fresh and fresh[0][0]:
            started = len([e for e in before if e[1] and e[0] == "ring" and not e[3]])
            usable = ("ring", 0, CHUNKS - 1, stages - 1) in before and started < 1
            usable = usable or ("ring", 0, CHUNKS - 1, stages) in before
        elif fresh:
            usable = True
        if event is None and usable and link - now < depth:
            event = ("ring", *fresh.pop(0), 0)
        if event is None:
            times = [item[0] + 1.5 * item[1][1] for item in waiting]
            if usable:
                times.append(link - depth + 0.01)
            now = max(now + 0.01, min(times))
            continue
        run(event)
        before.append(event)
        todo -= event[0] == "pair" and event[1] == 0
    clock = now + 1.3
    for it in range(NS_STEPS):
        for slot in range(SLOTS if it < NS_STEPS - 1 else 4):
            clock += step[slot]
            now = clock
            found = []
            while True:
                event = take(now - 0.3)
                if event is None and fresh and link - now < 2.0:
                    event = ("ring", *fresh.pop(0), 0)
                if event is None:
                    break
                run(event)
                found.append(event)
            clock = now
            slots[it, slot] = found
    while fresh or waiting:
        if fresh:
            event = ("ring", *fresh.pop(0), 0)
        else:
            event = take(min(item[0] for item in waiting))
        run(event)
        after.append(event)
    return before, slots, after


def dot_nt(lhs, rhs):
    return lax.dot_general(lhs, rhs, (((1,), (1,)), ((), ())), preferred_element_type=F32)


def dot_nn(lhs, rhs):
    return jnp.dot(lhs, rhs, preferred_element_type=F32)


def muon_kernel(
    dims, grad, mom, wgt, rate, decay, momv, wgtv, full,
    gown, gpar, ring, usend, xs0, xs1, xs2, aown, apar, bmat, xfin, xback, sums,
    own_sem, mw_sem, gp_s, gp_r, ring_s, ring_r, a2a_s, a2a_r, yg_s, yg_r, half_s, half_r,
    xe_s, xe_r, ae_s, ae_r, bk_s, bk_r, ag_s, ag_r, ad_s, ad_r,
):
    nx, tp, mats, rows, cols = dims
    waves = mats // nx
    piece = rows // CHUNKS
    half = nx * rows
    width = tp * cols
    blk = min(256, half // 2)
    nblk = min(256, cols // 2)
    xs = (xs0, xs1)
    pong = xs2
    out_scale = 0.2 * math.sqrt(max(2 * half, width))

    d = lax.axis_index("dp")
    y = lax.axis_index("tp")
    x = d // 2
    c = d % 2
    turn = 1 - 2 * c
    nxt_x = (x + turn + nx) % nx
    partner = {"dp": 2 * x + (1 - c)}
    right = {"dp": 2 * nxt_x + c}

    my_cols = pl.ds(pl.multiple_of(y * cols, cols), cols)

    def at_x(dx):
        return {"dp": 2 * ((x + dx) % nx) + c}

    def at_y(dy):
        return {"tp": (y + dy) % tp}

    def remote(src, dst, send, recv, dev):
        return pltpu.make_async_remote_copy(
            src_ref=src, dst_ref=dst, send_sem=send, recv_sem=recv, device_id=dev, device_id_type=MESH
        )

    def all_of(like, sem):
        pltpu.make_async_copy(like, like, sem).wait()

    def wave(w):
        return pl.ds(w * nx, nx)

    def part(q):
        return pl.ds(q * piece, piece)

    def own_load(w, q):
        return pltpu.make_async_copy(
            grad.at[wave(w), :, c, part(q)], gown.at[wave(w), :, part(q)], own_sem.at[w, q]
        )

    def pair_copy(w, q):
        return remote(
            grad.at[wave(w), :, 1 - c, part(q)], gpar.at[wave(w), :, part(q)], gp_s.at[0], gp_r.at[w, q], partner
        )

    mom_load = pltpu.make_async_copy(mom, momv, mw_sem.at[0])
    wgt_load = pltpu.make_async_copy(wgt, wgtv, mw_sem.at[1])
    for w in range(waves):
        for q in range(CHUNKS):
            own_load(w, q).start()
    mom_load.start()
    wgt_load.start()

    barrier = pltpu.get_barrier_semaphore()
    peers = [partner] + [at_x(dx) for dx in range(1, nx)] + [at_y(dy) for dy in range(1, tp)]
    for peer in peers:
        pl.semaphore_signal(barrier, inc=1, device_id=peer, device_id_type=MESH)
    pl.semaphore_wait(barrier, len(peers))
    for w in range(waves):
        for q in range(CHUNKS):
            pair_copy(w, q).start()

    def ring_block(stage):
        return (x - turn * (1 + stage) + 4 * nx) % nx

    def ring_copy(w, q, stage):
        if stage == 0:
            src = gown.at[wave(w), ring_block(0), part(q)]
        else:
            src = ring.at[w, q, stage - 1]
        return remote(src, ring.at[w, q, stage], ring_s.at[0], ring_r.at[w, q, stage], right)

    def a2a_copy(w, q, dx):
        owner = (x + dx) % nx
        return remote(
            usend.at[w * nx + owner, part(q)],
            xs[w].at[0, x, part(q), my_cols],
            a2a_s.at[0], a2a_r.at[w, q], at_x(dx),
        )

    def ring_event(w, q, stage):
        block = ring_block(stage)
        if stage == 0:
            own_load(w, q).wait()
            pair_copy(w, q).wait_recv()
        else:
            ring_copy(w, q, stage - 1).wait_recv()
        for i in range(nx):
            m = w * nx + i
            local = gown[m, block, part(q)] + gpar[m, block, part(q)]
            if stage == 0:
                gown[m, block, part(q)] = local
            elif stage < nx - 1:
                ring[w, q, stage - 1, i] = ring[w, q, stage - 1, i] + local
            else:
                grad_mean = (ring[w, q, stage - 1, i] + local) * (1.0 / (2 * nx))
                mom_new = MOMENTUM * momv[m, part(q)] + grad_mean
                momv[m, part(q)] = mom_new
                usend[m, part(q)] = (grad_mean + MOMENTUM * mom_new).astype(BF16)
        if stage < nx - 1:
            ring_copy(w, q, stage).start()
        else:
            for dx in (2, 1, 3):
                a2a_copy(w, q, dx).start()
            xs[w][0, x, part(q), my_cols] = usend[w * nx + x, part(q)]

    def gather_copy(w, q, dy):
        region = xs[w].at[0, :, part(q), my_cols]
        return remote(region, region, yg_s.at[w], yg_r.at[w, q], at_y(dy))

    def half_copy(w, q):
        return remote(
            xs[w].at[0, :, part(q)], xs[w].at[1, :, part(q)], half_s.at[w], half_r.at[w, q], partner
        )

    def gather_event(w, q):
        all_of(usend.at[pl.ds(0, nx - 1), part(q)], a2a_r.at[w, q])
        for dy in (2, 1, 3):
            if dy < tp:
                gather_copy(w, q, dy).start()

    def add_squares(w, side, q):
        acc = sums[w]
        for i in range(nx):
            v = xs[w][side, i, part(q), :].astype(F32)
            v = v * v
            for n in range(width // 128):
                acc = acc + v[:, n * 128:(n + 1) * 128]
        sums[w] = acc

    def half_event(w, q):
        all_of(xs[w].at[0, :, part(q), pl.ds(0, width - cols)], yg_r.at[w, q])
        half_copy(w, q).start()
        add_squares(w, 0, q)

    def pair_event(w, q):
        half_copy(w, q).wait_recv()
        add_squares(w, 1, q)

    def normalise(w):
        all_of(xs[w].at[0], half_s.at[w])
        all_of(xs[w].at[0, :, :, pl.ds(0, width - cols)], yg_s.at[w])
        total = jnp.sum(sums[w])
        inv = 1.0 / (jnp.sqrt(jnp.full((8, 128), total, F32)) + NORM_EPS)
        inv = inv[0:1, 0:1]

        def scale_rows(r, carry):
            sl = pl.ds(pl.multiple_of(r * 16, 16), 16)
            for side in range(2):
                for i in range(nx):
                    xs[w][side, i, sl, :] = (xs[w][side, i, sl, :].astype(F32) * inv).astype(BF16)
            return carry

        lax.fori_loop(0, rows // 16, scale_rows, 0)

    own = pl.ds(0, half)
    own_blocks = half // blk
    n_chunks = width // nblk
    batch = max(1, n_chunks // 2)

    def chunk_copy(dst, par, n):
        col = pl.ds(pl.multiple_of(n * nblk, nblk), nblk)
        return remote(dst.at[0, :, :, col], dst.at[1, :, :, col], xe_s.at[par], xe_r.at[par], partner)

    def newton_schulz(w, service):
        def a_copy(par):
            slot = (par + w) % 2
            return remote(aown.at[:, own], apar.at[slot], ae_s.at[slot], ae_r.at[slot], partner)

        def a_block(cur, side, j):
            per = blk // rows if blk >= rows else 1
            rhs = cur[side, j * per:(j + 1) * per].reshape(blk, width)
            lhs = cur[0].reshape(half, width)
            col = (side * own_blocks + j) * blk
            aown[:, col:col + blk] = dot_nt(lhs, rhs).astype(BF16)

        def b_own(j):
            rs = slice(j * blk, (j + 1) * blk)
            sq = dot_nt(aown[...], aown[rs, :])
            bmat[:, rs] = (COEF_B * aown[:, rs].astype(F32) + COEF_C * sq).astype(BF16)

        def b_other(par, j):
            rs = slice(j * blk, (j + 1) * blk)
            ps = slice(half + j * blk, half + (j + 1) * blk)
            sq = dot_nn(aown[:, :half], aown[:, ps]) + dot_nn(aown[:, half:], apar[(par + w) % 2, :, rs])
            bmat[:, ps] = (COEF_B * aown[:, ps].astype(F32) + COEF_C * sq).astype(BF16)

        def x_cols(cur, col):
            rhs = cur[:, :, :, col].reshape(2 * half, nblk)
            new = COEF_A * cur[0, :, :, col].reshape(half, nblk).astype(F32) + dot_nn(bmat[...], rhs)
            return new.astype(BF16)

        def iteration(it, par, cur, nxt, first, final):
            def drain_a():
                a_copy(1 - par).wait_send()

            def need_x():
                all_of(cur.at[0], xe_s.at[1 - par])
                all_of(cur.at[1], xe_r.at[1 - par])

            def guarded(fn):
                if first is False:
                    fn()
                else:
                    pl.when(jnp.logical_not(first))(fn)

            guarded(drain_a)
            for j in range(own_blocks):
                a_block(cur, 0, j)
            a_copy(par).start()
            service(it, 0)
            guarded(need_x)
            for j in range(own_blocks):
                a_block(cur, 1, j)
            service(it, 1)
            a_copy(par).wait_recv()
            for j in range(own_blocks):
                b_own(j)
            for j in range(own_blocks):
                b_other(par, j)
            service(it, 2)
            service(it, 3)
            if final:
                for n in range(cols // nblk):
                    col = pl.ds(pl.multiple_of(y * cols + n * nblk, nblk), nblk)
                    xfin[w, :, :, n * nblk:(n + 1) * nblk] = x_cols(cur, col).reshape(nx, rows, nblk)
            else:
                def x_pair(k, carry):
                    cols_of = [pl.ds(pl.multiple_of((2 * k + e) * nblk, nblk), nblk) for e in range(2)]
                    for col in cols_of:
                        nxt[0, :, :, col] = x_cols(cur, col).reshape(nx, rows, nblk)
                    for e in range(2):
                        chunk_copy(nxt, par, 2 * k + e).start()
                    return carry

                for part_no in range(2):
                    lax.fori_loop(part_no * batch // 2, (part_no + 1) * batch // 2, x_pair, 0)
                    service(it, 4 + part_no)

        def pair_of_steps(p, carry):
            iteration((p, 0), 0, xs[w], pong, p == 0, False)
            iteration((p, 1), 1, pong, xs[w], False, False)
            return carry

        lax.fori_loop(0, NS_STEPS // 2, pair_of_steps, 0)
        iteration(NS_STEPS - 1, 0, xs[w], None, False, True)
        a_copy(0).wait_send()

    def back_copy(w, dx):
        return remote(
            xfin.at[w, (x + dx) % nx],
            xback.at[w * nx + x], bk_s.at[0], bk_r.at[w, dx], at_x(dx),
        )

    def back_arrival(w, dx):
        m = w * nx + (x - dx + nx) % nx
        return remote(
            xfin.at[w, 0], xback.at[m], bk_s.at[0], bk_r.at[w, dx], at_x(dx)
        )

    def back_send(w):
        for dx in (1, 3, 2):
            back_copy(w, dx).start()
        xback[w * nx + x] = xfin[w, x]

    order = (0, 1, 3, 2)

    def gather_slot(w, hop, j):
        holder = (x - turn * hop + 4 * nx) % nx
        return holder, w * nx + (holder - order[j] + nx) % nx

    def ag_copy(w, hop, j):
        holder, m = gather_slot(w, hop, j)
        block = full.at[m, holder, c]
        return remote(block, block, ag_s.at[0], ag_r.at[m, hop], right)

    def ag_arrival(w, hop, j):
        holder, m = gather_slot(w, hop + 1, j)
        block = full.at[m, holder, c]
        return remote(block, block, ag_s.at[0], ag_r.at[m, hop], right)

    def pair_full(w, hop, j):
        holder, m = gather_slot(w, hop, j)
        block = full.at[m, holder, c]
        return remote(block, block, ad_s.at[0], ad_r.at[w], partner)

    def weight_event(w, j):
        dx = order[j]
        m = w * nx + (x - dx + nx) % nx
        if dx:
            back_arrival(w, dx).wait_recv()
        w_old = wgtv[m]
        w_new = w_old - rate[m] * (out_scale * xback[m].astype(F32) + decay[0] * w_old)
        wgtv[m] = w_new
        full[m, x, c] = w_new.astype(BF16)
        ag_copy(w, 0, j).start()
        pair_full(w, 0, j).start()

    def forward_event(w, hop, j):
        ag_arrival(w, hop - 1, j).wait_recv()
        if hop < nx - 1:
            ag_copy(w, hop, j).start()
        pair_full(w, hop, j).start()

    def finish_gather(w):
        all_of(full.at[wave(w), :, 1 - c], ad_r.at[w])

    handlers = {"ring": ring_event, "gather": gather_event, "half": half_event, "pair": pair_event}

    def perform(events):
        for kind, *rest in events:
            handlers[kind](*rest)

    def server(table):
        def service(it, slot):
            if isinstance(it, tuple):
                p, odd = it
                for k in range(NS_STEPS // 2):
                    work = table.get((2 * k + odd, slot), [])
                    if work:
                        pl.when(p == k)(functools.partial(perform, work))
            else:
                perform(table.get((it, slot), []))
        return service

    handlers["weight"] = weight_event
    handlers["forward"] = forward_event
    before, during, after = make_plan(waves, nx - 1)
    for w in range(waves):
        sums[w] = jnp.zeros((piece, 128), F32)
    mom_load.wait()
    perform(before)
    normalise(0)
    newton_schulz(0, server(during))
    back_send(0)
    wgt_load.wait()
    perform([e for e in after if e[0] in ("ring", "gather")])
    perform([("weight", 0, 0)])
    perform([e for e in after if e[0] in ("half", "pair")])
    normalise(1)
    second = {
        (0, 4): [("weight", 0, 1)], (0, 5): [("weight", 0, 2)], (1, 0): [("weight", 0, 3)],
        (1, 2): [("forward", 0, 1, 0)], (1, 3): [("forward", 0, 1, 1)],
        (1, 4): [("forward", 0, 1, 2)], (1, 5): [("forward", 0, 1, 3)],
        (2, 2): [("forward", 0, 2, 0)], (2, 3): [("forward", 0, 2, 1)],
        (2, 4): [("forward", 0, 2, 2)], (2, 5): [("forward", 0, 2, 3)],
        (3, 2): [("forward", 0, 3, 0)], (3, 3): [("forward", 0, 3, 1)],
        (3, 4): [("forward", 0, 3, 2)], (3, 5): [("forward", 0, 3, 3)],
    }
    newton_schulz(1, server(second))
    back_send(1)
    perform([("weight", 1, j) for j in range(nx)])
    perform([("forward", 1, hop, j) for hop in range(1, nx) for j in range(nx)])
    for w in range(waves):
        finish_gather(w)

    all_of(gpar, gp_s.at[0])
    all_of(ring, ring_s.at[0])
    all_of(usend.at[pl.ds(0, waves * (nx - 1))], a2a_s.at[0])
    all_of(xback.at[pl.ds(0, waves * (nx - 1))], bk_s.at[0])
    all_of(full.at[:, pl.ds(0, nx - 1), 0], ag_s.at[0])
    all_of(full.at[:, :, 0], ad_s.at[0])


def store_kernel(a, b, c, a_out, b_out, c_out, sem):
    cut = a.shape[0] // 2
    pieces = [(c.at[m], c_out.at[m]) for m in range(c.shape[0])]
    for src, dst in ((a, a_out), (b, b_out)):
        pieces += [(src.at[pl.ds(k * cut, cut)], dst.at[pl.ds(k * cut, cut)]) for k in range(2)]
    copies = [pltpu.make_async_copy(src, dst, sem.at[i]) for i, (src, dst) in enumerate(pieces)]
    for copy in copies:
        copy.start()
    for copy in copies:
        copy.wait()


def solution(mesh):
    dp = mesh.shape["dp"]
    tp = mesh.shape["tp"]
    nx = dp // 2

    def local_step(grad_local, mom_local, weight_local, learn_rate, decay_rate):
        mats, rows, cols = mom_local.shape
        waves = mats // nx
        piece = rows // CHUNKS
        half = nx * rows
        width = tp * cols
        n_chunks = width // min(256, cols // 2)
        dma = pltpu.SemaphoreType.DMA
        vmem = pltpu.VMEM
        anyspec = pl.BlockSpec(memory_space=pl.ANY)
        smem = pl.BlockSpec(memory_space=pltpu.SMEM)
        vspec = pl.BlockSpec(memory_space=pltpu.VMEM)
        grad_view = grad_local.reshape(mats, nx, 2, rows, cols)
        call = pl.pallas_call(
            functools.partial(muon_kernel, (nx, tp, mats, rows, cols)),
            out_shape=(
                vmem((mats, rows, cols), F32),
                vmem((mats, rows, cols), F32),
                vmem((mats, nx, 2, rows, cols), BF16),
            ),
            in_specs=[anyspec, anyspec, anyspec, smem, smem],
            out_specs=(vspec, vspec, vspec),
            scratch_shapes=[
                vmem((mats, nx, rows, cols), F32),
                vmem((mats, nx, rows, cols), F32),
                vmem((waves, CHUNKS, nx - 1, nx, piece, cols), F32),
                vmem((mats, rows, cols), BF16),
                vmem((2, nx, rows, width), BF16),
                vmem((2, nx, rows, width), BF16),
                vmem((2, nx, rows, width), BF16),
                vmem((half, 2 * half), BF16),
                vmem((2, half, half), BF16),
                vmem((half, 2 * half), BF16),
                vmem((waves, nx, rows, cols), BF16),
                vmem((mats, rows, cols), BF16),
                vmem((waves, piece, 128), F32),
                dma((waves, CHUNKS)),
                dma((2,)),
                dma((1,)),
                dma((waves, CHUNKS)),
                dma((1,)),
                dma((waves, CHUNKS, nx - 1)),
                dma((1,)),
                dma((waves, CHUNKS)),
                dma((waves,)),
                dma((waves, CHUNKS)),
                dma((waves,)),
                dma((waves, CHUNKS)),
                dma((2,)),
                dma((2,)),
                dma((2,)),
                dma((2,)),
                dma((1,)),
                dma((waves, nx)),
                dma((1,)),
                dma((mats, nx - 1)),
                dma((1,)),
                dma((waves,)),
            ],
            compiler_params=pltpu.CompilerParams(
                collective_id=0, has_side_effects=True, vmem_limit_bytes=46 * 1024 * 1024
            ),
        )
        results = call(grad_view, mom_local, weight_local, learn_rate, decay_rate.reshape(1))
        results = [pltpu.with_memory_space_constraint(r, pltpu.VMEM) for r in results]
        mom_new, weight_new, full = pl.pallas_call(
            store_kernel,
            out_shape=tuple(jax.ShapeDtypeStruct(r.shape, r.dtype) for r in results),
            in_specs=[vspec] * 3,
            out_specs=(anyspec,) * 3,
            scratch_shapes=[dma((mats + 4,))],
            compiler_params=pltpu.CompilerParams(vmem_limit_bytes=1024 * 1024),
        )(*results)
        return mom_new, weight_new, full.reshape(mats, dp * rows, cols)

    return jax.shard_map(
        local_step,
        mesh=mesh,
        in_specs=(P(("rep", "dp"), None, None, "tp"), P("rep", "dp", "tp"), P("rep", "dp", "tp"), P("rep"), P()),
        out_specs=(P("rep", "dp", "tp"), P("rep", "dp", "tp"), P("rep", None, "tp")),
        check_vma=False,
    )
```
